128 devices in a mesh: gx: 4 (over z_lo, core), gy: 4 (over y), gz: 8 (over x, z_hi).
Axes of the slice: x: 4, y: 4, z: 4 (z_hi: 2, z_lo: 2; z = z_hi * 2 + z_lo), core: 2. Of those that a mesh axis runs over, the one named last changes fastest.
Arguments:
- gradients: bfloat16 [128, 3072, 512], P(('gx', 'gy', 'gz')), may hold values from -24 to 24
- master_weights: float32 [3072, 512], P(('gx', 'gy', 'gz')), may hold values from -10 to 10
- first_moment: float32 [3072, 512], P(('gx', 'gy', 'gz')), may hold values from -8 to 8
- second_moment: float32 [3072, 512], P(('gx', 'gy', 'gz')), may hold values from 1 to 100
- tensor_ids: int32 [3072], P(('gx', 'gy', 'gz')), may hold values from 0 to 3, as said below
Outputs:
- new_master: float32 [3072, 512], P(('gx', 'gy', 'gz'))
- new_first: float32 [3072, 512], P(('gx', 'gy', 'gz'))
- new_second: float32 [3072, 512], P(('gx', 'gy', 'gz'))
- scaled_update: float32 [3072, 512], P(('gx', 'gy', 'gz'))
- params: bfloat16 [3072, 512], replicated
The draws below stay inside these ranges and needn't reach their ends.
Inputs may be any that keep to these rules, and one draw needn't show every extreme that they name: `tensor_ids`: nondecreasing along the rows; every tensor of 4 owns one contiguous run of rows.
All inputs are finite; a program needn't handle non-finite values.
Results may differ from the reference program's by a relative error of at most 0.0045.
Values may be sent and summed in bfloat16 or wider, within the bound.
No kernel may reach another device: no remote copies, remote signals or barrier semaphores. Data moves between devices by JAX's collectives and lax.ppermute only.
A program may use at most 64 MiB of HBM per device.

```python
import math
import jax
import jax.numpy as jnp
from jax import lax

COLS = 512
NT = 4
BROWS = 3072
DEVICES = 128


def tensor_layout(key):
    base_rows = BROWS // NT
    spread = BROWS // (4 * NT)
    shifts = jax.random.randint(jax.random.fold_in(key, 11), (NT - 1,), -spread, spread + 1).astype(jnp.int32)
    leading = base_rows + shifts
    last_rows = (BROWS - jnp.sum(leading)).astype(jnp.int32)
    lengths = jnp.concatenate([leading, last_rows[None]])
    starts = jnp.cumsum(lengths) - lengths
    row_index = jnp.arange(BROWS, dtype=jnp.int32)
    tensor_ids = jnp.sum((row_index[:, None] >= starts[None, 1:]).astype(jnp.int32), axis=1).astype(jnp.int32)
    scales = jnp.exp(jax.random.uniform(jax.random.fold_in(key, 12), (NT,), jnp.float32, math.log(0.25), math.log(2.0)))
    return (tensor_ids, scales)


def draw_tensor_ids(key, part):
    tensor_ids, scales = tensor_layout(key)
    return tensor_ids


def draw_master_weights(key, part):
    tensor_ids, scales = tensor_layout(key)
    row_scale = scales[tensor_ids][:, None]
    values = jnp.clip(jax.random.normal(jax.random.fold_in(key, 13), (BROWS, COLS), jnp.float32), -5.0, 5.0)
    return (values * row_scale).astype(jnp.float32)


def strengthened(drawn, rng, source, target, parts, factor):
    owner, partner = [(jnp.arange(drawn.shape[axis_at]) // (drawn.shape[axis_at] // parts)).reshape([-1 if axis == axis_at else 1 for axis in range(drawn.ndim)]) for axis_at in (source, target)]
    chosen = jax.random.permutation(rng, parts)[partner]
    strong = (owner == chosen) | (owner == (partner + parts // 2) % parts)
    return jnp.where(strong, factor * drawn, drawn)


def levels(stream_key, dims, shards, low, top_value):
    factor_of, own = 1.0, jax.random.fold_in(stream_key, 6)
    for dim, blocks in shards:
        steps = jnp.exp(jax.random.uniform(jax.random.fold_in(own, dim), (blocks,), jnp.float32, low / len(shards), top_value / len(shards)))
        factor_of = factor_of * jnp.repeat(steps, dims[dim] // blocks).reshape([-1 if axis == dim else 1 for axis in range(len(dims))])
    return factor_of


def scatter_about(own_key, extent, deviation, most, split=(), kind=jnp.bfloat16):
    result = jax.random.normal(own_key, extent, jnp.float32) * deviation
    if len(split) > 0:
        result = levels(own_key, extent, split, -0.22, 0.18) * result
    return jnp.clip(result, min=-most, max=most).astype(kind)


def bell_draw_with(rng, shape, width, bound, pieces, heavy, kind=jnp.bfloat16):
    result = width * jax.random.normal(rng, shape, jnp.float32)
    if pieces:
        result = result * levels(rng, shape, pieces, -0.22, 0.18)
    return jnp.clip(strengthened(result, jax.random.fold_in(rng, 3), *heavy), -bound, bound).astype(kind)


def setup_inputs(seed: int = 0) -> dict:
    key_of = jax.random.split(jax.random.key(seed), 6)
    gradients = bell_draw_with(key_of[0], (DEVICES, BROWS, COLS), 1.0, 24.0, ((0, 128),), (0, 1, 128, 5.5))
    master_weights = draw_master_weights(jax.random.fold_in(key_of[5], 71), 0)
    first_moment = scatter_about(key_of[2], (BROWS, COLS), 2.0, 8.0, ((0, 128),), jnp.float32)
    second_moment = jnp.clip(jnp.exp(math.log(100.0) - 4.6051702 * jax.random.uniform(key_of[3], (BROWS, COLS), jnp.float32) ** levels(key_of[3], (BROWS, COLS), ((0, 128),), -0.2, 0.2)), 1.0, 100.0)
    tensor_ids = draw_tensor_ids(jax.random.fold_in(key_of[5], 71), 0)
    return {"gradients": gradients, "master_weights": master_weights, "first_moment": first_moment, "second_moment": second_moment, "tensor_ids": tensor_ids}


decay_first = 0.9
decay_second = 0.999
epsilon = 1e-06
weight_decay = 0.01
step_size = 0.05

def tensor_sums(values, onehot):
    return jnp.dot(lax.optimization_barrier(jnp.sum(values * values, axis=1)), onehot, precision=lax.Precision.HIGHEST)

def reference(gradients, master_weights, first_moment, second_moment, tensor_ids):
    summed = lax.optimization_barrier(jnp.sum(gradients.astype(jnp.float32), axis=0))
    new_first = decay_first * first_moment + (1.0 - decay_first) * summed
    new_second = decay_second * second_moment + (1.0 - decay_second) * summed * summed
    update = new_first / (jnp.sqrt(new_second) + epsilon) + weight_decay * master_weights
    onehot = (tensor_ids[:, None] == jnp.arange(NT, dtype=jnp.int32)[None, :]).astype(jnp.float32)
    weight_sq = tensor_sums(master_weights, onehot)
    update_sq = tensor_sums(update, onehot)
    counts = lax.optimization_barrier(jnp.sum(onehot, axis=0)) * COLS
    trust_ratio = jnp.sqrt(weight_sq / (update_sq + counts))
    row_trust = jnp.dot(onehot, trust_ratio, precision=lax.Precision.HIGHEST)
    scaled_update = row_trust[:, None] * update
    new_master = master_weights - step_size * scaled_update
    params = new_master.astype(jnp.bfloat16)
    return (new_master, new_first, new_second, scaled_update, params)
```

```python
import functools

import jax
import jax.numpy as jnp
import numpy as np
from jax import lax
from jax.experimental import pallas as pl
from jax.experimental.pallas import tpu as pltpu
from jax.sharding import Mesh
from jax.sharding import PartitionSpec as P

decay_first = 0.9
decay_second = 0.999
epsilon = 1e-06
weight_decay = 0.01
step_size = 0.05


ROWS = 24
COLS = 512
CHIPS = 64
GROUP = 8
F32 = jnp.float32
BF16 = jnp.bfloat16

NUMBER = np.arange(2 * CHIPS).reshape(2, 2, 4, 4, 2)
PLACE = NUMBER.transpose(3, 2, 4, 0, 1).reshape(4, 4, 4, 2)

ALL_CHIPS = [NUMBER[:, core].reshape(CHIPS).tolist() for core in range(2)]
CORE_SWAP = [(int(a), int(b)) for pair in PLACE.reshape(CHIPS, 2) for a, b in (pair, pair[::-1])]


def grouping():
    wide, narrow = [], []
    for high in range(2):
        for z in range(4):
            wide.append([PLACE[x, 2 * high + low, z, 0] for x in range(4) for low in range(2)])
    for x in range(4):
        for low in range(2):
            narrow.append([PLACE[x, 2 * high + low, z, 0] for high in range(2) for z in range(4)])
    for x in range(4):
        for pair in ((2, 1), (0, 3)):
            wide.append([PLACE[x, pair[low], z, 1] for z in range(4) for low in range(2)])
    for z in range(4):
        for low in range(2):
            narrow.append([PLACE[x, 2 * high + low, z, 1] for x in range(4) for high in range(2)])
    as_ints = lambda groups: [[int(i) for i in group] for group in groups]
    return as_ints(wide), as_ints(narrow)


WIDE, NARROW = grouping()


def owners():
    table = np.zeros((2, GROUP, GROUP), np.int32)
    place_a = np.zeros(2 * CHIPS, np.int32)
    for group in WIDE:
        for a, device in enumerate(group):
            place_a[device] = a
    for group in NARROW:
        for b, device in enumerate(group):
            table[(device // 32) % 2, place_a[device], b] = device
    return table, place_a


OWNER, PLACE_A = owners()


def exchange(value, groups):
    return lax.all_to_all(value, "i", 0, 0, axis_index_groups=groups, tiled=True)


def lane_index(rows):
    return lax.broadcasted_iota(jnp.int32, (rows, 128), 1)


def update_kernel(parts, weights, first, second, ids, new_first, new_second, update, sums):
    summed = parts[0].astype(F32)
    for k in range(1, CHIPS):
        summed = summed + parts[k].astype(F32)
    w = weights[...]
    m = decay_first * first[...] + (1.0 - decay_first) * summed
    v = decay_second * second[...] + (1.0 - decay_second) * summed * summed
    u = m / (jnp.sqrt(v) + epsilon) + weight_decay * w
    new_first[...] = m
    new_second[...] = v
    update[...] = u
    lane = lane_index(ROWS)
    kind = lane // 4
    w_sq = jnp.sum(w * w, axis=1, keepdims=True)
    u_sq = jnp.sum(u * u, axis=1, keepdims=True)
    by_kind = jnp.where(kind == 0, w_sq, jnp.where(kind == 1, u_sq, jnp.where(kind == 2, float(COLS), 0.0)))
    per_tensor = jnp.sum(jnp.where(ids[...] == lane % 4, by_kind, 0.0), axis=0, keepdims=True)
    sums[...] = jnp.broadcast_to(per_tensor, (8, 128))


PAY = 2 * ROWS + 8


def pay_kernel(update, weights, sums, pay):
    total = sums[0, 0:1, :]
    for k in range(1, GROUP):
        total = total + sums[k, 0:1, :]
    high = total.astype(BF16)
    rest = total - high.astype(F32)
    mid = rest.astype(BF16)
    low = (rest - mid.astype(F32)).astype(BF16)
    row = lax.broadcasted_iota(jnp.int32, (8, 128), 0)
    three = jnp.where(
        row == 0, high.astype(F32), jnp.where(row == 1, mid.astype(F32), jnp.where(row == 2, low.astype(F32), 0.0))
    )
    three = jnp.concatenate([three, jnp.zeros((8, COLS - 128), F32)], axis=1)
    one = jnp.concatenate([update[...], weights[...], three], axis=0).astype(BF16)
    for k in range(GROUP):
        pay[k] = one


def trust_and_runs(got):
    total = jnp.zeros((1, 128), F32)
    for k in range(GROUP):
        three = got[k, 2 * ROWS :, 0:128].astype(F32)
        total = total + ((three[0:1] + three[1:2]) + three[2:3])
    update_sq = pltpu.roll(total, 124, 1)
    count = pltpu.roll(total, 120, 1)
    lane = lane_index(1)
    used = lane < 4
    trust = jnp.where(used, jnp.sqrt(total / (update_sq + count)), 0.0)
    rows = jnp.where(used, count * (1.0 / COLS), 0.0)
    start = jnp.zeros((1, 128), F32)
    for k in range(1, 4):
        start = start + jnp.where(lane >= k, pltpu.roll(rows, k, 1), 0.0)
    return trust, start, jnp.where(used, start + rows, -1.0)


def row_trust(first_row, trust, start, end):
    row = (lax.broadcasted_iota(jnp.int32, (ROWS, 128), 0) + first_row).astype(F32)
    here = jnp.logical_and(row >= start, row < end)
    return jnp.sum(jnp.where(here, trust, 0.0), axis=1, keepdims=True)


def params_kernel(owner, got, params):
    trust, start, end = trust_and_runs(got)
    for b in range(GROUP):
        factor = row_trust(owner[b] * ROWS, trust, start, end)
        update = got[b, 0:ROWS].astype(F32)
        weights = got[b, ROWS : 2 * ROWS].astype(F32)
        block = (weights - step_size * (factor * update)).astype(BF16)
        for a in range(GROUP):
            params[a, b] = block


def own_rows_kernel(me, got, update, weights, new_master, scaled_update):
    trust, start, end = trust_and_runs(got)
    scaled = row_trust(me[0] * ROWS, trust, start, end) * update[...]
    scaled_update[...] = scaled
    new_master[...] = weights[...] - step_size * scaled


def place_kernel(owner, blocks, out, done):
    def start(k, carry):
        pltpu.make_async_copy(blocks.at[k], out.at[owner[k]], done).start()
        return carry

    lax.fori_loop(0, CHIPS, start, 0, unroll=True)
    pltpu.make_async_copy(blocks, out.at[pl.ds(0, CHIPS)], done).wait()


def place_more_kernel(owner, blocks, before, out, done):
    del before
    place_kernel(owner, blocks, out, done)


SMEM = pl.BlockSpec(memory_space=pltpu.SMEM)
VMEM = pl.BlockSpec(memory_space=pltpu.VMEM)
ANY = pl.BlockSpec(memory_space=pl.ANY)


def of(shape, dtype):
    return jax.ShapeDtypeStruct(shape, dtype)


def on_device(gradients, master_weights, first_moment, second_moment, tensor_ids):
    me = lax.axis_index("i")
    core = (me // 32) % 2
    own_f32 = of((ROWS, COLS), F32)

    halves = gradients.reshape(2, 2, CHIPS // 2 * ROWS, COLS)
    kept = lax.dynamic_index_in_dim(halves, core, 1, keepdims=False)
    sent = lax.dynamic_index_in_dim(halves, 1 - core, 1, keepdims=False)
    arrived = lax.ppermute(sent, "i", CORE_SWAP)
    both = (kept.astype(F32) + arrived.astype(F32)).astype(BF16)
    parts = exchange(both.reshape(CHIPS, ROWS, COLS), ALL_CHIPS)

    new_first, new_second, update, sums = pl.pallas_call(
        update_kernel,
        out_shape=(own_f32, own_f32, own_f32, of((8, 128), F32)),
        in_specs=[VMEM] * 5,
        out_specs=(VMEM,) * 4,
        name="lamb_update",
    )(parts, master_weights, first_moment, second_moment, tensor_ids.reshape(ROWS, 1))

    sums = sums + lax.ppermute(sums, "i", CORE_SWAP)
    sums = exchange(jnp.broadcast_to(sums[None], (GROUP, 8, 128)), WIDE)
    pay = pl.pallas_call(
        pay_kernel,
        out_shape=of((GROUP, PAY, COLS), BF16),
        in_specs=[VMEM] * 3,
        out_specs=VMEM,
        name="pay",
    )(update, master_weights, sums)
    got = exchange(pay, NARROW)

    owner = jnp.asarray(OWNER)
    mine = owner[core].reshape(CHIPS)
    others = owner[1 - core].reshape(CHIPS)
    place = jnp.asarray(PLACE_A)[me]
    params = pl.pallas_call(
        params_kernel,
        out_shape=of((GROUP, GROUP, ROWS, COLS), BF16),
        in_specs=[SMEM, VMEM],
        out_specs=VMEM,
        name="params",
    )(lax.dynamic_slice(mine, (place * GROUP,), (GROUP,)), got)
    wide = exchange(params, WIDE).reshape(CHIPS, ROWS, COLS)
    new_master, scaled_update = pl.pallas_call(
        own_rows_kernel,
        out_shape=(own_f32, own_f32),
        in_specs=[SMEM, VMEM, VMEM, VMEM],
        out_specs=(VMEM, VMEM),
        name="own_rows",
    )(me.reshape(1), got, update, master_weights)
    swapped = lax.ppermute(wide, "i", CORE_SWAP)
    gathered = pl.pallas_call(
        place_kernel,
        out_shape=of((2 * CHIPS, ROWS, COLS), BF16),
        in_specs=[SMEM, ANY],
        out_specs=ANY,
        scratch_shapes=[pltpu.SemaphoreType.DMA],
        name="place_own",
    )(mine, wide)
    gathered = pl.pallas_call(
        place_more_kernel,
        out_shape=of((2 * CHIPS, ROWS, COLS), BF16),
        in_specs=[SMEM, ANY, ANY],
        out_specs=ANY,
        scratch_shapes=[pltpu.SemaphoreType.DMA],
        input_output_aliases={2: 0},
        name="place_other",
    )(others, swapped, gathered)
    return (new_master, new_first, new_second, scaled_update, gathered.reshape(2 * CHIPS * ROWS, COLS))


def solution(mesh):
    flat = Mesh(mesh.devices.reshape(2 * CHIPS), ("i",))
    return jax.shard_map(
        on_device,
        mesh=flat,
        in_specs=(P("i", None, None), P("i", None), P("i", None), P("i", None), P("i")),
        out_specs=(P("i", None), P("i", None), P("i", None), P("i", None), P()),
        check_vma=False,
    )
```

```python
import functools

import jax
import jax.numpy as jnp
import numpy as np
from jax import lax
from jax.experimental import pallas as pl
from jax.experimental.pallas import tpu as pltpu
from jax.sharding import Mesh
from jax.sharding import PartitionSpec as P

decay_first = 0.9
decay_second = 0.999
epsilon = 1e-06
weight_decay = 0.01
step_size = 0.05


ROWS = 24
COLS = 512
CHIPS = 64
GROUP = 8
F32 = jnp.float32
BF16 = jnp.bfloat16

NUMBER = np.arange(2 * CHIPS).reshape(2, 2, 4, 4, 2)
PLACE = NUMBER.transpose(3, 2, 4, 0, 1).reshape(4, 4, 4, 2)

ALL_CHIPS = [NUMBER[:, core].reshape(CHIPS).tolist() for core in range(2)]
CORE_SWAP = [(int(a), int(b)) for pair in PLACE.reshape(CHIPS, 2) for a, b in (pair, pair[::-1])]


def grouping():
    wide, narrow = [], []
    for high in range(2):
        for z in range(4):
            wide.append([PLACE[x, 2 * high + low, z, 0] for x in range(4) for low in range(2)])
    for x in range(4):
        for low in range(2):
            narrow.append([PLACE[x, 2 * high + low, z, 0] for high in range(2) for z in range(4)])
    for x in range(4):
        for pair in ((2, 1), (0, 3)):
            wide.append([PLACE[x, pair[low], z, 1] for z in range(4) for low in range(2)])
    for z in range(4):
        for low in range(2):
            narrow.append([PLACE[x, 2 * high + low, z, 1] for x in range(4) for high in range(2)])
    as_ints = lambda groups: [[int(i) for i in group] for group in groups]
    return as_ints(wide), as_ints(narrow)


WIDE, NARROW = grouping()


def place_of(device):
    return device >> 6, (device >> 5) & 1, (device >> 3) & 3, (device >> 1) & 3, device & 1


def wide_place(device):
    z_lo, core, y, x, z_hi = place_of(device)
    return jnp.where(core == 0, x, 2 * z_hi + z_lo) * 2 + (y & 1)


def owner_of(core, a, b):
    first = core == 0
    x = jnp.where(first, a >> 1, b >> 1)
    z = jnp.where(first, b & 3, a >> 1)
    y = (a & 1) + 2 * jnp.where(first, b >> 2, b & 1)
    return ((z & 1) << 6) + (core << 5) + (y << 3) + (x << 1) + (z >> 1)


def exchange(value, groups):
    return lax.all_to_all(value, "i", 0, 0, axis_index_groups=groups, tiled=True)


def lane_index(rows):
    return lax.broadcasted_iota(jnp.int32, (rows, 128), 1)


def update_kernel(parts, weights, first, second, ids, new_first, new_second, update, sums):
    summed = parts[0].astype(F32)
    for k in range(1, CHIPS):
        summed = summed + parts[k].astype(F32)
    w = weights[...]
    m = decay_first * first[...] + (1.0 - decay_first) * summed
    v = decay_second * second[...] + (1.0 - decay_second) * summed * summed
    u = m / (jnp.sqrt(v) + epsilon) + weight_decay * w
    new_first[...] = m
    new_second[...] = v
    update[...] = u
    lane = lane_index(ROWS)
    kind = lane // 4
    w_sq = jnp.sum(w * w, axis=1, keepdims=True)
    u_sq = jnp.sum(u * u, axis=1, keepdims=True)
    by_kind = jnp.where(kind == 0, w_sq, jnp.where(kind == 1, u_sq, jnp.where(kind == 2, float(COLS), 0.0)))
    per_tensor = jnp.sum(jnp.where(ids[...] == lane % 4, by_kind, 0.0), axis=0, keepdims=True)
    sums[...] = jnp.broadcast_to(per_tensor, (8, 128))


PAY = 2 * ROWS + 8


def pay_kernel(update, weights, sums, pay):
    total = sums[0, 0:1, :]
    for k in range(1, GROUP):
        total = total + sums[k, 0:1, :]
    high = total.astype(BF16)
    rest = total - high.astype(F32)
    mid = rest.astype(BF16)
    low = (rest - mid.astype(F32)).astype(BF16)
    row = lax.broadcasted_iota(jnp.int32, (8, 128), 0)
    three = jnp.where(
        row == 0, high.astype(F32), jnp.where(row == 1, mid.astype(F32), jnp.where(row == 2, low.astype(F32), 0.0))
    )
    three = jnp.concatenate([three, jnp.zeros((8, COLS - 128), F32)], axis=1)
    one = jnp.concatenate([update[...], weights[...], three], axis=0).astype(BF16)
    for k in range(GROUP):
        pay[k] = one


def trust_and_runs(got):
    total = jnp.zeros((1, 128), F32)
    for k in range(GROUP):
        three = got[k, 2 * ROWS :, 0:128].astype(F32)
        total = total + ((three[0:1] + three[1:2]) + three[2:3])
    update_sq = pltpu.roll(total, 124, 1)
    count = pltpu.roll(total, 120, 1)
    lane = lane_index(1)
    used = lane < 4
    trust = jnp.where(used, jnp.sqrt(total / (update_sq + count)), 0.0)
    rows = jnp.where(used, count * (1.0 / COLS), 0.0)
    start = jnp.zeros((1, 128), F32)
    for k in range(1, 4):
        start = start + jnp.where(lane >= k, pltpu.roll(rows, k, 1), 0.0)
    return trust, start, jnp.where(used, start + rows, -1.0)


def row_trust(first_row, trust, start, end):
    row = (lax.broadcasted_iota(jnp.int32, (ROWS, 128), 0) + first_row).astype(F32)
    here = jnp.logical_and(row >= start, row < end)
    return jnp.sum(jnp.where(here, trust, 0.0), axis=1, keepdims=True)


def params_kernel(me, got, params):
    trust, start, end = trust_and_runs(got)
    core = (me[0] >> 5) & 1
    place = wide_place(me[0])
    for b in range(GROUP):
        factor = row_trust(owner_of(core, place, b) * ROWS, trust, start, end)
        update = got[b, 0:ROWS].astype(F32)
        weights = got[b, ROWS : 2 * ROWS].astype(F32)
        block = (weights - step_size * (factor * update)).astype(BF16)
        for a in range(GROUP):
            params[a, b] = block


def own_rows_kernel(me, got, update, weights, new_master, scaled_update):
    trust, start, end = trust_and_runs(got)
    scaled = row_trust(me[0] * ROWS, trust, start, end) * update[...]
    scaled_update[...] = scaled
    new_master[...] = weights[...] - step_size * scaled


def take_kernel(me, gradients, half, done, *, other):
    core = (me[0] >> 5) & 1
    if other:
        core = 1 - core
    copies = [
        pltpu.make_async_copy(gradients.at[z_lo, core], half.at[pl.ds(z_lo * CHIPS // 2, CHIPS // 2)], done.at[z_lo])
        for z_lo in range(2)
    ]
    for copy in copies:
        copy.start()
    for copy in copies:
        copy.wait()


def add_kernel(kept, arrived, both):
    def add(k, carry):
        both[k] = kept[k] + arrived[k]
        return carry

    lax.fori_loop(0, CHIPS, add, 0, unroll=8)


def chip_sums_kernel(sums, arrived, out):
    both = sums[...] + arrived[...]
    for k in range(GROUP):
        out[k] = both


def place_blocks(core, blocks, out, done):
    for a in range(GROUP):
        for b in range(GROUP):
            pltpu.make_async_copy(blocks.at[a * GROUP + b], out.at[owner_of(core, a, b)], done).start()
    pltpu.make_async_copy(blocks, out.at[pl.ds(0, CHIPS)], done).wait()


def place_kernel(me, blocks, out, done):
    place_blocks((me[0] >> 5) & 1, blocks, out, done)


def place_more_kernel(me, blocks, before, out, done):
    del before
    place_blocks(1 - ((me[0] >> 5) & 1), blocks, out, done)


SMEM = pl.BlockSpec(memory_space=pltpu.SMEM)
VMEM = pl.BlockSpec(memory_space=pltpu.VMEM)
HBM = pl.BlockSpec(memory_space=pltpu.HBM)


def of(shape, dtype):
    return jax.ShapeDtypeStruct(shape, dtype)


def kernel(body, name, ins, outs, shapes, limit=8, **more):
    return pl.pallas_call(
        body,
        out_shape=shapes,
        in_specs=ins,
        out_specs=outs,
        compiler_params=pltpu.CompilerParams(vmem_limit_bytes=limit * 2**20),
        name=name,
        **more,
    )


def on_device(gradients, master_weights, first_moment, second_moment, tensor_ids):
    me = lax.axis_index("i").astype(jnp.int32).reshape(1)
    own_f32 = of((ROWS, COLS), F32)
    half = pltpu.VMEM((CHIPS, ROWS, COLS), BF16)
    copy_scratch = dict(scratch_shapes=[pltpu.SemaphoreType.DMA((2,))])

    halves = gradients.reshape(2, 2, CHIPS // 2, ROWS, COLS)
    take = lambda other, name: kernel(
        functools.partial(take_kernel, other=other), name, [SMEM, HBM], VMEM, half, **copy_scratch
    )(me, halves)
    sent = take(True, "take_sent")
    arrived = lax.ppermute(sent, "i", CORE_SWAP)
    kept = take(False, "take_kept")
    both = kernel(add_kernel, "add_cores", [VMEM] * 2, VMEM, half)(kept, arrived)
    parts = exchange(both, ALL_CHIPS)

    new_first, new_second, update, sums = kernel(
        update_kernel, "lamb_update", [VMEM] * 5, (VMEM,) * 4, (own_f32, own_f32, own_f32, of((8, 128), F32))
    )(parts, master_weights, first_moment, second_moment, tensor_ids.reshape(ROWS, 1))

    arrived = lax.ppermute(sums, "i", CORE_SWAP)
    sums = kernel(chip_sums_kernel, "chip_sums", [VMEM] * 2, VMEM, of((GROUP, 8, 128), F32))(sums, arrived)
    sums = exchange(sums, WIDE)
    pay = kernel(pay_kernel, "pay", [VMEM] * 3, VMEM, of((GROUP, PAY, COLS), BF16))(update, master_weights, sums)
    got = exchange(pay, NARROW)

    params = kernel(params_kernel, "params", [SMEM, VMEM], VMEM, of((GROUP, GROUP, ROWS, COLS), BF16))(me, got)
    wide = exchange(params, WIDE).reshape(CHIPS, ROWS, COLS)
    new_master, scaled_update = kernel(own_rows_kernel, "own_rows", [SMEM] + [VMEM] * 3, (VMEM, VMEM), (own_f32, own_f32))(
        me, got, update, master_weights
    )
    swapped = lax.ppermute(wide, "i", CORE_SWAP)
    every = of((2 * CHIPS, ROWS, COLS), BF16)
    copy_scratch = dict(scratch_shapes=[pltpu.SemaphoreType.DMA])
    gathered = kernel(place_kernel, "place_own", [SMEM, VMEM], HBM, every, **copy_scratch)(me, wide)
    gathered = kernel(
        place_more_kernel, "place_other", [SMEM, VMEM, HBM], HBM, every, input_output_aliases={2: 0}, **copy_scratch
    )(me, swapped, gathered)
    gathered = gathered.reshape(2 * CHIPS * ROWS, COLS)
    return (new_master, new_first, new_second, scaled_update, gathered)


def solution(mesh):
    flat = Mesh(mesh.devices.reshape(2 * CHIPS), ("i",))
    return jax.shard_map(
        on_device,
        mesh=flat,
        in_specs=(P("i", None, None), P("i", None), P("i", None), P("i", None), P("i")),
        out_specs=(P("i", None), P("i", None), P("i", None), P("i", None), P()),
        check_vma=False,
    )
```

```python
import functools

import jax
import jax.numpy as jnp
import numpy as np
from jax import lax
from jax.experimental import pallas as pl
from jax.experimental.pallas import tpu as pltpu
from jax.sharding import Mesh
from jax.sharding import PartitionSpec as P

decay_first = 0.9
decay_second = 0.999
epsilon = 1e-06
weight_decay = 0.01
step_size = 0.05


ROWS = 24
COLS = 512
CHIPS = 64
GROUP = 8
F32 = jnp.float32
BF16 = jnp.bfloat16

NUMBER = np.arange(2 * CHIPS).reshape(2, 2, 4, 4, 2)
PLACE = NUMBER.transpose(3, 2, 4, 0, 1).reshape(4, 4, 4, 2)

CORE_SWAP = [(int(a), int(b)) for pair in PLACE.reshape(CHIPS, 2) for a, b in (pair, pair[::-1])]


def grouping():
    grid = np.zeros((2, GROUP, GROUP), int)
    for core in range(2):
        for a in range(GROUP):
            for b in range(GROUP):
                x, low, z, high = (a >> 1, a & 1, b >> 1, b & 1) if core == 0 else (b >> 1, b & 1, a >> 1, a & 1)
                grid[core, a, b] = PLACE[x, 2 * high + (low ^ high), z, core]
    wide = [grid[core, :, b].tolist() for core in range(2) for b in range(GROUP)]
    narrow = [grid[core, a, :].tolist() for core in range(2) for a in range(GROUP)]
    return wide, narrow


WIDE, NARROW = grouping()


def place_of(device):
    return device >> 6, (device >> 5) & 1, (device >> 3) & 3, (device >> 1) & 3, device & 1


def wide_place(device):
    z_lo, core, y, x, z_hi = place_of(device)
    return jnp.where(core == 0, 2 * x + ((y ^ (y >> 1)) & 1), 2 * (2 * z_hi + z_lo) + (y >> 1))


def owner_of(core, a, b):
    first = core == 0
    p = jnp.where(first, a, b)
    q = jnp.where(first, b, a)
    x, z = p >> 1, q >> 1
    y = 2 * (q & 1) + ((p ^ q) & 1)
    return ((z & 1) << 6) + (core << 5) + (y << 3) + (x << 1) + (z >> 1)


def exchange(value, groups):
    return lax.all_to_all(value, "i", 0, 0, axis_index_groups=groups, tiled=True)


def lane_index(rows):
    return lax.broadcasted_iota(jnp.int32, (rows, 128), 1)


def update_kernel(parts, weights, first, second, ids, new_first, new_second, update, sums):
    summed = parts[0].astype(F32)
    for k in range(1, GROUP):
        summed = summed + parts[k].astype(F32)
    w = weights[...]
    m = decay_first * first[...] + (1.0 - decay_first) * summed
    v = decay_second * second[...] + (1.0 - decay_second) * summed * summed
    u = m / (jnp.sqrt(v) + epsilon) + weight_decay * w
    new_first[...] = m
    new_second[...] = v
    update[...] = u
    lane = lane_index(ROWS)
    kind = lane // 4
    w_sq = jnp.sum(w * w, axis=1, keepdims=True)
    u_sq = jnp.sum(u * u, axis=1, keepdims=True)
    by_kind = jnp.where(kind == 0, w_sq, jnp.where(kind == 1, u_sq, jnp.where(kind == 2, float(COLS), 0.0)))
    row = lax.broadcasted_iota(jnp.int32, (ROWS, 128), 0)
    tensor = jnp.zeros((ROWS, 128), jnp.int32)
    for k in range(ROWS):
        tensor = jnp.where(row == k, ids[k], tensor)
    per_tensor = jnp.sum(jnp.where(tensor == lane % 4, by_kind, 0.0), axis=0, keepdims=True)
    sums[...] = jnp.broadcast_to(per_tensor, (8, 128))


PAY = 2 * ROWS + 8


def pay_kernel(update, weights, sums, pay):
    total = sums[0, 0:1, :]
    for k in range(1, GROUP):
        total = total + sums[k, 0:1, :]
    high = total.astype(BF16)
    rest = total - high.astype(F32)
    mid = rest.astype(BF16)
    low = (rest - mid.astype(F32)).astype(BF16)
    row = lax.broadcasted_iota(jnp.int32, (8, 128), 0)
    three = jnp.where(
        row == 0, high.astype(F32), jnp.where(row == 1, mid.astype(F32), jnp.where(row == 2, low.astype(F32), 0.0))
    )
    three = jnp.concatenate([three, jnp.zeros((8, COLS - 128), F32)], axis=1)
    one = jnp.concatenate([update[...], weights[...], three], axis=0).astype(BF16)
    for k in range(GROUP):
        pay[k] = one


def trust_and_runs(got):
    total = jnp.zeros((1, 128), F32)
    for k in range(GROUP):
        three = got[k, 2 * ROWS :, 0:128].astype(F32)
        total = total + ((three[0:1] + three[1:2]) + three[2:3])
    update_sq = pltpu.roll(total, 124, 1)
    count = pltpu.roll(total, 120, 1)
    lane = lane_index(1)
    used = lane < 4
    trust = jnp.where(used, jnp.sqrt(total / (update_sq + count)), 0.0)
    rows = jnp.where(used, count * (1.0 / COLS), 0.0)
    start = jnp.zeros((1, 128), F32)
    for k in range(1, 4):
        start = start + jnp.where(lane >= k, pltpu.roll(rows, k, 1), 0.0)
    return trust, start, jnp.where(used, start + rows, -1.0)


def row_trust(first_row, trust, start, end):
    row = (lax.broadcasted_iota(jnp.int32, (ROWS, 128), 0) + first_row).astype(F32)
    here = jnp.logical_and(row >= start, row < end)
    return jnp.sum(jnp.where(here, trust, 0.0), axis=1, keepdims=True)


def params_kernel(me, got, params):
    trust, start, end = trust_and_runs(got)
    core = (me[0] >> 5) & 1
    place = wide_place(me[0])
    for b in range(GROUP):
        factor = row_trust(owner_of(core, place, b) * ROWS, trust, start, end)
        update = got[b, 0:ROWS].astype(F32)
        weights = got[b, ROWS : 2 * ROWS].astype(F32)
        block = (weights - step_size * (factor * update)).astype(BF16)
        for a in range(GROUP):
            params[a, b] = block


def own_rows_kernel(me, got, update, weights, new_master, scaled_update):
    trust, start, end = trust_and_runs(got)
    scaled = row_trust(me[0] * ROWS, trust, start, end) * update[...]
    scaled_update[...] = scaled
    new_master[...] = weights[...] - step_size * scaled


def take_kernel(me, gradients, half, done, *, other):
    core = (me[0] >> 5) & 1
    if other:
        core = 1 - core
    copies = [
        pltpu.make_async_copy(gradients.at[z_lo, core], half.at[pl.ds(z_lo * CHIPS // 2, CHIPS // 2)], done.at[z_lo])
        for z_lo in range(2)
    ]
    for copy in copies:
        copy.start()
    for copy in copies:
        copy.wait()


def add_kernel(me, kept, arrived, both):
    core = (me[0] >> 5) & 1

    def add(a, carry):
        for b in range(GROUP):
            device = owner_of(core, a, b)
            k = ((device >> 6) << 5) + (device & 31)
            both[a, b] = kept[k] + arrived[k]
        return carry

    lax.fori_loop(0, GROUP, add, 0)


def total_kernel(parts, total):
    for b in range(GROUP):
        summed = parts[0, b].astype(F32)
        for a in range(1, GROUP):
            summed = summed + parts[a, b].astype(F32)
        total[b] = summed.astype(BF16)


def chip_sums_kernel(sums, arrived, out):
    both = sums[...] + arrived[...]
    for k in range(GROUP):
        out[k] = both


def place_blocks(core, blocks, out, done):
    for a in range(GROUP):
        for b in range(GROUP):
            pltpu.make_async_copy(blocks.at[a * GROUP + b], out.at[owner_of(core, a, b)], done).start()
    pltpu.make_async_copy(blocks, out.at[pl.ds(0, CHIPS)], done).wait()


def place_kernel(me, blocks, out, done):
    place_blocks((me[0] >> 5) & 1, blocks, out, done)


def place_more_kernel(me, blocks, before, out, done):
    del before
    place_blocks(1 - ((me[0] >> 5) & 1), blocks, out, done)


SMEM = pl.BlockSpec(memory_space=pltpu.SMEM)
VMEM = pl.BlockSpec(memory_space=pltpu.VMEM)
HBM = pl.BlockSpec(memory_space=pltpu.HBM)


def of(shape, dtype):
    return jax.ShapeDtypeStruct(shape, dtype)


def kernel(body, name, ins, outs, shapes, limit=8, **more):
    return pl.pallas_call(
        body,
        out_shape=shapes,
        in_specs=ins,
        out_specs=outs,
        compiler_params=pltpu.CompilerParams(vmem_limit_bytes=limit * 2**20),
        name=name,
        **more,
    )


def on_device(gradients, master_weights, first_moment, second_moment, tensor_ids):
    me = lax.axis_index("i").astype(jnp.int32).reshape(1)
    own_f32 = of((ROWS, COLS), F32)
    half = pltpu.VMEM((CHIPS, ROWS, COLS), BF16)
    copy_scratch = dict(scratch_shapes=[pltpu.SemaphoreType.DMA((2,))])

    halves = gradients.reshape(2, 2, CHIPS // 2, ROWS, COLS)
    halves = pltpu.with_memory_space_constraint(halves, pltpu.HBM)
    take = lambda other, name: kernel(
        functools.partial(take_kernel, other=other), name, [SMEM, HBM], VMEM, half, **copy_scratch
    )(me, halves)
    sent = take(True, "take_sent")
    arrived = lax.ppermute(sent, "i", CORE_SWAP)
    kept = take(False, "take_kept")
    blocks = pltpu.VMEM((GROUP, GROUP, ROWS, COLS), BF16)
    both = kernel(add_kernel, "add_cores", [SMEM] + [VMEM] * 2, VMEM, blocks)(me, kept, arrived)
    parts = exchange(both, WIDE)
    total = kernel(total_kernel, "add_wide", [VMEM], VMEM, pltpu.VMEM((GROUP, ROWS, COLS), BF16))(parts)
    parts = exchange(total, NARROW)

    new_first, new_second, update, sums = kernel(
        update_kernel, "lamb_update", [VMEM] * 4 + [SMEM], (VMEM,) * 4, (own_f32, own_f32, own_f32, of((8, 128), F32))
    )(parts, master_weights, first_moment, second_moment, tensor_ids)

    arrived = lax.ppermute(sums, "i", CORE_SWAP)
    sums = kernel(chip_sums_kernel, "chip_sums", [VMEM] * 2, VMEM, of((GROUP, 8, 128), F32))(sums, arrived)
    sums = exchange(sums, WIDE)
    pay = kernel(pay_kernel, "pay", [VMEM] * 3, VMEM, of((GROUP, PAY, COLS), BF16))(update, master_weights, sums)
    got = exchange(pay, NARROW)

    params = kernel(params_kernel, "params", [SMEM, VMEM], VMEM, of((GROUP, GROUP, ROWS, COLS), BF16))(me, got)
    wide = exchange(params, WIDE).reshape(CHIPS, ROWS, COLS)
    new_master, scaled_update = kernel(own_rows_kernel, "own_rows", [SMEM] + [VMEM] * 3, (VMEM, VMEM), (own_f32, own_f32))(
        me, got, update, master_weights
    )
    swapped = lax.ppermute(wide, "i", CORE_SWAP)
    every = of((2 * CHIPS, ROWS, COLS), BF16)
    copy_scratch = dict(scratch_shapes=[pltpu.SemaphoreType.DMA])
    gathered = kernel(place_kernel, "place_own", [SMEM, VMEM], HBM, every, **copy_scratch)(me, wide)
    gathered = kernel(
        place_more_kernel, "place_other", [SMEM, VMEM, HBM], HBM, every, input_output_aliases={2: 0}, **copy_scratch
    )(me, swapped, gathered)
    gathered = gathered.reshape(2 * CHIPS * ROWS, COLS)
    return (new_master, new_first, new_second, scaled_update, gathered)


def solution(mesh):
    flat = Mesh(mesh.devices.reshape(2 * CHIPS), ("i",))
    return jax.shard_map(
        on_device,
        mesh=flat,
        in_specs=(P("i", None, None), P("i", None), P("i", None), P("i", None), P("i")),
        out_specs=(P("i", None), P("i", None), P("i", None), P("i", None), P()),
        check_vma=False,
    )
```

```python
import functools

import jax
import jax.numpy as jnp
import numpy as np
from jax import lax
from jax.experimental import pallas as pl
from jax.experimental.pallas import tpu as pltpu
from jax.sharding import Mesh
from jax.sharding import PartitionSpec as P


decay_first = 0.9
decay_second = 0.999
epsilon = 1e-06
weight_decay = 0.01
step_size = 0.05


ROWS = 24
COLS = 512
CHIPS = 64
GROUP = 8
F32 = jnp.float32
BF16 = jnp.bfloat16

NUMBER = np.arange(2 * CHIPS).reshape(2, 2, 4, 4, 2)
PLACE = NUMBER.transpose(3, 2, 4, 0, 1).reshape(4, 4, 4, 2)

CORE_SWAP = [(int(a), int(b)) for pair in PLACE.reshape(CHIPS, 2) for a, b in (pair, pair[::-1])]


def grouping():
    grid = np.zeros((2, GROUP, GROUP), int)
    for core in range(2):
        for a in range(GROUP):
            for b in range(GROUP):
                x, low, z, high = (a >> 1, a & 1, b >> 1, b & 1) if core == 0 else (b >> 1, b & 1, a >> 1, a & 1)
                grid[core, a, b] = PLACE[x, 2 * high + (low ^ high), z, core]
    wide = [grid[core, :, b].tolist() for core in range(2) for b in range(GROUP)]
    narrow = [grid[core, a, :].tolist() for core in range(2) for a in range(GROUP)]
    return wide, narrow


WIDE, NARROW = grouping()


def place_of(device):
    return device >> 6, (device >> 5) & 1, (device >> 3) & 3, (device >> 1) & 3, device & 1


def wide_place(device):
    z_lo, core, y, x, z_hi = place_of(device)
    return jnp.where(core == 0, 2 * x + ((y ^ (y >> 1)) & 1), 2 * (2 * z_hi + z_lo) + (y >> 1))


OFFSETS = ((2, 1), (3, 1), (1, 1), (2, 0), (0, 1), (3, 0), (1, 0))


def source_place(a, offset):
    ring, pair = offset
    return ((((a >> 1) + 4 - ring) & 3) << 1) + ((a & 1) ^ pair)


def wide_shift(offset):
    return [(group[source_place(a, offset)], group[a]) for group in WIDE for a in range(GROUP)]


def owner_of(core, a, b):
    first = core == 0
    p = jnp.where(first, a, b)
    q = jnp.where(first, b, a)
    x, z = p >> 1, q >> 1
    y = 2 * (q & 1) + ((p ^ q) & 1)
    return ((z & 1) << 6) + (core << 5) + (y << 3) + (x << 1) + (z >> 1)


def exchange(value, groups):
    return lax.all_to_all(value, "i", 0, 0, axis_index_groups=groups, tiled=True)


def lane_index(rows):
    return lax.broadcasted_iota(jnp.int32, (rows, 128), 1)


def update_kernel(parts, weights, first, second, ids, new_first, new_second, update, sums):
    summed = parts[0].astype(F32)
    for k in range(1, GROUP):
        summed = summed + parts[k].astype(F32)
    w = weights[...]
    m = decay_first * first[...] + (1.0 - decay_first) * summed
    v = decay_second * second[...] + (1.0 - decay_second) * summed * summed
    u = m / (jnp.sqrt(v) + epsilon) + weight_decay * w
    new_first[...] = m
    new_second[...] = v
    update[...] = u
    lane = lane_index(ROWS)
    kind = lane // 4
    w_sq = jnp.sum(w * w, axis=1, keepdims=True)
    u_sq = jnp.sum(u * u, axis=1, keepdims=True)
    by_kind = jnp.where(kind == 0, w_sq, jnp.where(kind == 1, u_sq, jnp.where(kind == 2, float(COLS), 0.0)))
    row = lax.broadcasted_iota(jnp.int32, (ROWS, 128), 0)
    tensor = jnp.zeros((ROWS, 128), jnp.int32)
    for k in range(ROWS):
        tensor = jnp.where(row == k, ids[k], tensor)
    per_tensor = jnp.sum(jnp.where(tensor == lane % 4, by_kind, 0.0), axis=0, keepdims=True)
    sums[...] = jnp.broadcast_to(per_tensor, (8, 128))


PAY = 2 * ROWS + 8


def pay_kernel(update, weights, sums, pay):
    total = sums[0, 0:1, :]
    for k in range(1, GROUP):
        total = total + sums[k, 0:1, :]
    high = total.astype(BF16)
    rest = total - high.astype(F32)
    mid = rest.astype(BF16)
    low = (rest - mid.astype(F32)).astype(BF16)
    row = lax.broadcasted_iota(jnp.int32, (8, 128), 0)
    three = jnp.where(
        row == 0, high.astype(F32), jnp.where(row == 1, mid.astype(F32), jnp.where(row == 2, low.astype(F32), 0.0))
    )
    three = jnp.concatenate([three, jnp.zeros((8, COLS - 128), F32)], axis=1)
    one = jnp.concatenate([update[...], weights[...], three], axis=0).astype(BF16)
    for k in range(GROUP):
        pay[k] = one


def trust_and_runs(got):
    total = jnp.zeros((1, 128), F32)
    for k in range(GROUP):
        three = got[k, 2 * ROWS :, 0:128].astype(F32)
        total = total + ((three[0:1] + three[1:2]) + three[2:3])
    update_sq = pltpu.roll(total, 124, 1)
    count = pltpu.roll(total, 120, 1)
    lane = lane_index(1)
    used = lane < 4
    trust = jnp.where(used, jnp.sqrt(total / (update_sq + count)), 0.0)
    rows = jnp.where(used, count * (1.0 / COLS), 0.0)
    start = jnp.zeros((1, 128), F32)
    for k in range(1, 4):
        start = start + jnp.where(lane >= k, pltpu.roll(rows, k, 1), 0.0)
    return trust, start, jnp.where(used, start + rows, -1.0)


def row_trust(first_row, trust, start, end):
    row = (lax.broadcasted_iota(jnp.int32, (ROWS, 128), 0) + first_row).astype(F32)
    here = jnp.logical_and(row >= start, row < end)
    return jnp.sum(jnp.where(here, trust, 0.0), axis=1, keepdims=True)


def params_kernel(me, got, params):
    trust, start, end = trust_and_runs(got)
    core = (me[0] >> 5) & 1
    place = wide_place(me[0])
    for b in range(GROUP):
        factor = row_trust(owner_of(core, place, b) * ROWS, trust, start, end)
        update = got[b, 0:ROWS].astype(F32)
        weights = got[b, ROWS : 2 * ROWS].astype(F32)
        params[b] = (weights - step_size * (factor * update)).astype(BF16)


def own_rows_kernel(me, got, update, weights, new_master, scaled_update):
    trust, start, end = trust_and_runs(got)
    scaled = row_trust(me[0] * ROWS, trust, start, end) * update[...]
    scaled_update[...] = scaled
    new_master[...] = weights[...] - step_size * scaled


def take_kernel(me, gradients, half, done, *, other):
    core = (me[0] >> 5) & 1
    if other:
        core = 1 - core
    copies = [
        pltpu.make_async_copy(gradients.at[z_lo, core], half.at[pl.ds(z_lo * CHIPS // 2, CHIPS // 2)], done.at[z_lo])
        for z_lo in range(2)
    ]
    for copy in copies:
        copy.start()
    for copy in copies:
        copy.wait()


def add_kernel(me, kept, arrived, both):
    core = (me[0] >> 5) & 1

    def add(a, carry):
        for b in range(GROUP):
            device = owner_of(core, a, b)
            k = ((device >> 6) << 5) + (device & 31)
            both[a, b] = kept[k] + arrived[k]
        return carry

    lax.fori_loop(0, GROUP, add, 0)


def total_kernel(parts, total):
    for b in range(GROUP):
        summed = parts[0, b].astype(F32)
        for a in range(1, GROUP):
            summed = summed + parts[a, b].astype(F32)
        total[b] = summed.astype(BF16)


def chip_sums_kernel(sums, arrived, out):
    both = sums[...] + arrived[...]
    for k in range(GROUP):
        out[k] = both


def join_kernel(*refs):
    for k, part in enumerate(refs[:-1]):
        refs[-1][k] = part[...]


def place_kernel(me, *refs, chunks, first):
    count = 1 + max(chunk[0] for chunk in chunks)
    blocks, out, done = refs[:count], refs[-2], refs[-1]
    del first
    for array, index, other, offset in chunks:
        device = me[0] ^ (32 if other else 0)
        core = (device >> 5) & 1
        a = source_place(wide_place(device), offset)
        part = blocks[array] if index is None else blocks[array].at[index]
        for b in range(GROUP):
            pltpu.make_async_copy(part.at[b], out.at[owner_of(core, a, b)], done).start()
    total = len(chunks) * GROUP
    pltpu.make_async_copy(out.at[pl.ds(0, total)], out.at[pl.ds(0, total)], done).wait()


SMEM = pl.BlockSpec(memory_space=pltpu.SMEM)
VMEM = pl.BlockSpec(memory_space=pltpu.VMEM)
HBM = pl.BlockSpec(memory_space=pltpu.HBM)


def of(shape, dtype):
    return jax.ShapeDtypeStruct(shape, dtype)


def kernel(body, ins, outs, shapes, limit=8, **more):
    return pl.pallas_call(
        body,
        out_shape=shapes,
        in_specs=ins,
        out_specs=outs,
        compiler_params=pltpu.CompilerParams(vmem_limit_bytes=limit * 2**20),
        **more,
    )


def on_device(gradients, master_weights, first_moment, second_moment, tensor_ids):
    me = lax.axis_index("i").astype(jnp.int32).reshape(1)
    own_f32 = of((ROWS, COLS), F32)
    half = pltpu.VMEM((CHIPS, ROWS, COLS), BF16)
    copy_scratch = dict(scratch_shapes=[pltpu.SemaphoreType.DMA((2,))])

    halves = gradients.reshape(2, 2, CHIPS // 2, ROWS, COLS)
    halves = pltpu.with_memory_space_constraint(halves, pltpu.HBM)
    take = lambda other: kernel(
        functools.partial(take_kernel, other=other), [SMEM, HBM], VMEM, half, **copy_scratch
    )(me, halves)
    sent = take(True)
    arrived = lax.ppermute(sent, "i", CORE_SWAP)
    kept = take(False)
    blocks = pltpu.VMEM((GROUP, GROUP, ROWS, COLS), BF16)
    both = kernel(add_kernel, [SMEM] + [VMEM] * 2, VMEM, blocks)(me, kept, arrived)
    parts = exchange(both, WIDE)
    total = kernel(total_kernel, [VMEM], VMEM, pltpu.VMEM((GROUP, ROWS, COLS), BF16))(parts)
    parts = exchange(total, NARROW)

    new_first, new_second, update, sums = kernel(
        update_kernel, [VMEM] * 4 + [SMEM], (VMEM,) * 4, (own_f32, own_f32, own_f32, of((8, 128), F32))
    )(parts, master_weights, first_moment, second_moment, tensor_ids)

    arrived = lax.ppermute(sums, "i", CORE_SWAP)
    sums = kernel(chip_sums_kernel, [VMEM] * 2, VMEM, of((GROUP, 8, 128), F32))(sums, arrived)
    sums = exchange(sums, WIDE)
    pay = kernel(pay_kernel, [VMEM] * 3, VMEM, of((GROUP, PAY, COLS), BF16))(update, master_weights, sums)
    got = exchange(pay, NARROW)

    chunk = pltpu.VMEM((GROUP, ROWS, COLS), BF16)
    params = kernel(params_kernel, [SMEM, VMEM], VMEM, chunk)(me, got)
    new_master, scaled_update = kernel(
        own_rows_kernel, [SMEM] + [VMEM] * 3, (VMEM, VMEM), (own_f32, own_f32)
    )(me, got, update, master_weights)

    def send(value, pairs):
        return lax.ppermute(value, "i", pairs)

    join = lambda *parts: kernel(
        join_kernel, [VMEM] * len(parts), VMEM, pltpu.VMEM((len(parts), GROUP, ROWS, COLS), BF16)
    )(*parts)
    every = of((2 * CHIPS, ROWS, COLS), BF16)

    def place(arrays, chunks, before=None):
        first = before is None
        return kernel(
            functools.partial(place_kernel, chunks=chunks, first=first),
            [SMEM] + [VMEM] * len(arrays) + ([] if first else [HBM]),
            HBM,
            every,
            scratch_shapes=[pltpu.SemaphoreType.DMA],
            input_output_aliases={} if first else {1 + len(arrays): 0},
        )(me, *arrays, *(() if first else (before,)))

    own = (0, 0)
    wide = [send(params, wide_shift(offset)) for offset in OFFSETS]
    other_own = send(params, CORE_SWAP)
    other_0 = send(join(*wide[0:3]), CORE_SWAP)
    other_1 = send(join(*wide[3:5]), CORE_SWAP)
    other_2 = send(wide[5], CORE_SWAP)
    other_3 = send(wide[6], CORE_SWAP)
    gathered = place(
        [params, *wide[0:5], other_own, other_0],
        [(0, None, False, own)]
        + [(1 + k, None, False, OFFSETS[k]) for k in range(5)]
        + [(6, None, True, own)]
        + [(7, k, True, OFFSETS[k]) for k in range(3)],
    )
    gathered = place(
        [wide[5], other_1], [(0, None, False, OFFSETS[5])] + [(1, k, True, OFFSETS[3 + k]) for k in range(2)], gathered
    )
    gathered = place(
        [wide[6], other_2, other_3],
        [(0, None, False, OFFSETS[6]), (1, None, True, OFFSETS[5]), (2, None, True, OFFSETS[6])],
        gathered,
    )
    gathered = gathered.reshape(2 * CHIPS * ROWS, COLS)
    return (new_master, new_first, new_second, scaled_update, gathered)


def solution(mesh):
    flat = Mesh(mesh.devices.reshape(2 * CHIPS), ("i",))
    return jax.shard_map(
        on_device,
        mesh=flat,
        in_specs=(P("i", None, None), P("i", None), P("i", None), P("i", None), P("i")),
        out_specs=(P("i", None), P("i", None), P("i", None), P("i", None), P()),
        check_vma=False,
    )
```

```python
import functools

import jax
import jax.numpy as jnp
import numpy as np
from jax import lax
from jax.experimental import pallas as pl
from jax.experimental.pallas import tpu as pltpu
from jax.sharding import Mesh
from jax.sharding import PartitionSpec as P


decay_first = 0.9
decay_second = 0.999
epsilon = 1e-06
weight_decay = 0.01
step_size = 0.05


ROWS = 24
COLS = 512
CHIPS = 64
GROUP = 8
F32 = jnp.float32
BF16 = jnp.bfloat16

NUMBER = np.arange(2 * CHIPS).reshape(2, 2, 4, 4, 2)
PLACE = NUMBER.transpose(3, 2, 4, 0, 1).reshape(4, 4, 4, 2)

CORE_SWAP = [(int(a), int(b)) for pair in PLACE.reshape(CHIPS, 2) for a, b in (pair, pair[::-1])]


def grouping():
    grid = np.zeros((2, GROUP, GROUP), int)
    for core in range(2):
        for a in range(GROUP):
            for b in range(GROUP):
                x, low, z, high = (a >> 1, a & 1, b >> 1, b & 1) if core == 0 else (b >> 1, b & 1, a >> 1, a & 1)
                grid[core, a, b] = PLACE[x, 2 * high + (low ^ high), z, core]
    wide = [grid[core, :, b].tolist() for core in range(2) for b in range(GROUP)]
    narrow = [grid[core, a, :].tolist() for core in range(2) for a in range(GROUP)]
    return wide, narrow


WIDE, NARROW = grouping()


def place_of(device):
    return device >> 6, (device >> 5) & 1, (device >> 3) & 3, (device >> 1) & 3, device & 1


def wide_place(device):
    z_lo, core, y, x, z_hi = place_of(device)
    return jnp.where(core == 0, 2 * x + ((y ^ (y >> 1)) & 1), 2 * (2 * z_hi + z_lo) + (y >> 1))


OFFSETS = ((2, 1), (3, 1), (1, 1), (2, 0), (0, 1), (3, 0), (1, 0))
OWN = (0, 0)


def source_place(a, offset):
    ring, pair = offset
    return ((((a >> 1) + 4 - ring) & 3) << 1) + ((a & 1) ^ pair)


def target_place(a, offset):
    ring, pair = offset
    return ((((a >> 1) + ring) & 3) << 1) + ((a & 1) ^ pair)


def wide_shift(offset):
    return [(group[source_place(a, offset)], group[a]) for group in WIDE for a in range(GROUP)]


def owner_of(core, a, b):
    first = core == 0
    p = jnp.where(first, a, b)
    q = jnp.where(first, b, a)
    x, z = p >> 1, q >> 1
    y = 2 * (q & 1) + ((p ^ q) & 1)
    return ((z & 1) << 6) + (core << 5) + (y << 3) + (x << 1) + (z >> 1)


def exchange(value, groups):
    return lax.all_to_all(value, "i", 0, 0, axis_index_groups=groups, tiled=True)


def lane_index(rows):
    return lax.broadcasted_iota(jnp.int32, (rows, 128), 1)


def before_kernel(weights, ids, tensor, sums):
    row = lax.broadcasted_iota(jnp.int32, (ROWS, 128), 0)
    of_row = jnp.zeros((ROWS, 128), jnp.int32)
    for k in range(ROWS):
        of_row = jnp.where(row == k, ids[k], of_row)
    tensor[...] = of_row
    lane = lane_index(ROWS)
    kind = lane // 4
    w = weights[...]
    w_sq = jnp.sum(w * w, axis=1, keepdims=True)
    by_kind = jnp.where(kind == 0, w_sq, jnp.where(kind == 2, float(COLS), 0.0))
    per_tensor = jnp.sum(jnp.where(of_row == lane % 4, by_kind, 0.0), axis=0, keepdims=True)
    sums[...] = jnp.broadcast_to(per_tensor, (8, 128))


def update_kernel(parts, weights, first, second, tensor, base, new_first, new_second, update, sums):
    summed = parts[0].astype(F32)
    for k in range(1, GROUP):
        summed = summed + parts[k].astype(F32)
    m = decay_first * first[...] + (1.0 - decay_first) * summed
    v = decay_second * second[...] + (1.0 - decay_second) * summed * summed
    u = m / (jnp.sqrt(v) + epsilon) + weight_decay * weights[...]
    new_first[...] = m
    new_second[...] = v
    update[...] = u
    u_sq = jnp.sum(u * u, axis=1, keepdims=True)
    here = tensor[...] + 4 == lane_index(ROWS)
    per_tensor = jnp.sum(jnp.where(here, u_sq, 0.0), axis=0, keepdims=True)
    sums[...] = base[...] + jnp.broadcast_to(per_tensor, (8, 128))


PAY = 2 * ROWS + 8


def pay_kernel(update, weights, sums, pay):
    total = sums[0, 0:1, :]
    for k in range(1, GROUP):
        total = total + sums[k, 0:1, :]
    high = total.astype(BF16)
    rest = total - high.astype(F32)
    mid = rest.astype(BF16)
    low = (rest - mid.astype(F32)).astype(BF16)
    row = lax.broadcasted_iota(jnp.int32, (8, 128), 0)
    three = jnp.where(
        row == 0, high.astype(F32), jnp.where(row == 1, mid.astype(F32), jnp.where(row == 2, low.astype(F32), 0.0))
    )
    three = jnp.concatenate([three, jnp.zeros((8, COLS - 128), F32)], axis=1)
    one = jnp.concatenate([update[...], weights[...], three], axis=0).astype(BF16)
    for k in range(GROUP):
        pay[k] = one


def trust_and_runs(got):
    total = jnp.zeros((1, 128), F32)
    for k in range(GROUP):
        three = got[k, 2 * ROWS :, 0:128].astype(F32)
        total = total + ((three[0:1] + three[1:2]) + three[2:3])
    update_sq = pltpu.roll(total, 124, 1)
    count = pltpu.roll(total, 120, 1)
    lane = lane_index(1)
    used = lane < 4
    trust = jnp.where(used, jnp.sqrt(total / (update_sq + count)), 0.0)
    rows = jnp.where(used, count * (1.0 / COLS), 0.0)
    start = jnp.zeros((1, 128), F32)
    for k in range(1, 4):
        start = start + jnp.where(lane >= k, pltpu.roll(rows, k, 1), 0.0)
    return trust, start, jnp.where(used, start + rows, -1.0)


def row_trust(first_row, trust, start, end):
    row = (lax.broadcasted_iota(jnp.int32, (ROWS, 128), 0) + first_row).astype(F32)
    here = jnp.logical_and(row >= start, row < end)
    return jnp.sum(jnp.where(here, trust, 0.0), axis=1, keepdims=True)


def params_kernel(me, got, update, weights, params, new_master, scaled_update):
    trust, start, end = trust_and_runs(got)
    core = (me[0] >> 5) & 1
    place = wide_place(me[0])
    for b in range(GROUP):
        factor = row_trust(owner_of(core, place, b) * ROWS, trust, start, end)
        block = got[b, ROWS : 2 * ROWS].astype(F32) - step_size * (factor * got[b, 0:ROWS].astype(F32))
        params[b] = block.astype(BF16)
    scaled = row_trust(me[0] * ROWS, trust, start, end) * update[...]
    scaled_update[...] = scaled
    new_master[...] = weights[...] - step_size * scaled


def take_kernel(me, gradients, taken, done, *, other, offsets):
    device = me[0] ^ (32 if other else 0)
    core = (device >> 5) & 1
    for j, offset in enumerate(offsets):
        a = target_place(wide_place(device), offset)
        for b in range(GROUP):
            pltpu.make_async_copy(gradients.at[owner_of(core, a, b)], taken.at[j, b], done).start()
    pltpu.make_async_copy(taken, taken, done).wait()


def add_kernel(kept, arrived, *both):
    for j, out in enumerate(both):
        out[...] = kept[j] + arrived[j]


def total_kernel(*refs):
    for b in range(GROUP):
        summed = refs[0][b].astype(F32)
        for part in refs[1:-1]:
            summed = summed + part[b].astype(F32)
        refs[-1][b] = summed.astype(BF16)


def chip_sums_kernel(sums, arrived, out):
    both = sums[...] + arrived[...]
    for k in range(GROUP):
        out[k] = both


def join_kernel(*refs):
    for k, part in enumerate(refs[:-1]):
        refs[-1][k] = part[...]


def place_kernel(me, *refs, arrays, chunks, rows=0):
    blocks, whole = refs[:arrays], refs[arrays : arrays + rows]
    scratch = 1 + (rows > 0)
    outs = refs[len(refs) - scratch - 1 - rows : len(refs) - scratch]
    out, done = outs[0], refs[len(refs) - scratch]
    copies = [pltpu.make_async_copy(whole[k], outs[1 + k], refs[-1].at[k]) for k in range(rows)]
    for array, index, other, offset in chunks:
        device = me[0] ^ (32 if other else 0)
        core = (device >> 5) & 1
        a = source_place(wide_place(device), offset)
        part = blocks[array] if index is None else blocks[array].at[index]
        for b in range(GROUP):
            pltpu.make_async_copy(part.at[b], out.at[owner_of(core, a, b)], done).start()
    for copy in copies:
        copy.start()
    total = len(chunks) * GROUP
    pltpu.make_async_copy(out.at[pl.ds(0, total)], out.at[pl.ds(0, total)], done).wait()
    for copy in copies:
        copy.wait()


SMEM = pl.BlockSpec(memory_space=pltpu.SMEM)
VMEM = pl.BlockSpec(memory_space=pltpu.VMEM)
HBM = pl.BlockSpec(memory_space=pltpu.HBM)


def of(shape, dtype):
    return jax.ShapeDtypeStruct(shape, dtype)


def kernel(body, ins, outs, shapes, limit=8, **more):
    return pl.pallas_call(
        body,
        out_shape=shapes,
        in_specs=ins,
        out_specs=outs,
        compiler_params=pltpu.CompilerParams(vmem_limit_bytes=limit * 2**20),
        **more,
    )


def on_device(gradients, master_weights, first_moment, second_moment, tensor_ids):
    me = lax.axis_index("i").astype(jnp.int32).reshape(1)
    own_f32 = pltpu.VMEM((ROWS, COLS), F32)
    chunk = pltpu.VMEM((GROUP, ROWS, COLS), BF16)
    copied = dict(scratch_shapes=[pltpu.SemaphoreType.DMA])

    def send(value, pairs):
        return lax.ppermute(value, "i", pairs)

    blocks = pltpu.with_memory_space_constraint(gradients.reshape(2 * CHIPS, ROWS, COLS), pltpu.HBM)
    halves = (OFFSETS[:4], OFFSETS[4:] + (OWN,))

    def take(other, offsets):
        body = functools.partial(take_kernel, other=other, offsets=offsets)
        return kernel(body, [SMEM, HBM], VMEM, pltpu.VMEM((4, GROUP, ROWS, COLS), BF16), **copied)(me, blocks)

    sent = [take(True, offsets) for offsets in halves]
    arrived = [send(sent[k], CORE_SWAP) for k in range(2)]
    kept = [take(False, offsets) for offsets in halves]
    chunks = []
    for k in range(2):
        chunks += kernel(add_kernel, [VMEM] * 2, [VMEM] * 4, [chunk] * 4)(kept[k], arrived[k])
    tensor, sums = kernel(
        before_kernel, [VMEM, SMEM], (VMEM, VMEM), (pltpu.VMEM((ROWS, 128), jnp.int32), pltpu.VMEM((8, 128), F32))
    )(master_weights, tensor_ids)
    wide = [send(chunks[k], wide_shift(offset)) for k, offset in enumerate(OFFSETS)]
    total = kernel(total_kernel, [VMEM] * 8, VMEM, chunk)(chunks[7], *wide)
    parts = exchange(total, NARROW)

    new_first, new_second, update, sums = kernel(
        update_kernel, [VMEM] * 6, (VMEM,) * 4, (own_f32, own_f32, own_f32, pltpu.VMEM((8, 128), F32))
    )(parts, master_weights, first_moment, second_moment, tensor, sums)

    arrived = lax.ppermute(sums, "i", CORE_SWAP)
    sums = kernel(chip_sums_kernel, [VMEM] * 2, VMEM, pltpu.VMEM((GROUP, 8, 128), F32))(sums, arrived)
    sums = exchange(sums, WIDE)
    pay = kernel(pay_kernel, [VMEM] * 3, VMEM, pltpu.VMEM((GROUP, PAY, COLS), BF16))(update, master_weights, sums)
    got = exchange(pay, NARROW)

    params, new_master, scaled_update = kernel(
        params_kernel, [SMEM] + [VMEM] * 3, (VMEM,) * 3, (chunk, own_f32, own_f32)
    )(me, got, update, master_weights)
    join = lambda *parts: kernel(
        join_kernel, [VMEM] * len(parts), VMEM, pltpu.VMEM((len(parts), GROUP, ROWS, COLS), BF16)
    )(*parts)
    every = of((2 * CHIPS, ROWS, COLS), BF16)

    def place(arrays, chunks, before=None, rows=()):
        first = before is None
        count = len(arrays) + len(rows)
        return kernel(
            functools.partial(place_kernel, arrays=len(arrays), chunks=chunks, rows=len(rows)),
            [SMEM] + [VMEM] * count + ([] if first else [HBM]),
            [HBM] * (1 + len(rows)),
            [every] + [of((ROWS, COLS), F32)] * len(rows),
            input_output_aliases={} if first else {1 + count: 0},
            scratch_shapes=[pltpu.SemaphoreType.DMA] + ([pltpu.SemaphoreType.DMA((len(rows),))] if rows else []),
        )(me, *arrays, *rows, *(() if first else (before,)))

    wide = [send(params, wide_shift(offset)) for offset in OFFSETS]
    other_0 = send(join(params, *wide[0:3]), CORE_SWAP)
    other_1 = send(join(*wide[3:5]), CORE_SWAP)
    other_2 = send(join(*wide[5:7]), CORE_SWAP)
    gathered, new_first, new_second, new_master, scaled_update = place(
        [params, *wide[0:5], other_0],
        [(0, None, False, OWN)]
        + [(1 + k, None, False, OFFSETS[k]) for k in range(5)]
        + [(6, 0, True, OWN)]
        + [(6, 1 + k, True, OFFSETS[k]) for k in range(3)],
        rows=(new_first, new_second, new_master, scaled_update),
    )
    (gathered,) = place(
        [*wide[5:7], other_1, other_2],
        [(k, None, False, OFFSETS[5 + k]) for k in range(2)]
        + [(2, k, True, OFFSETS[3 + k]) for k in range(2)]
        + [(3, k, True, OFFSETS[5 + k]) for k in range(2)],
        gathered,
    )
    gathered = gathered.reshape(2 * CHIPS * ROWS, COLS)
    return (new_master, new_first, new_second, scaled_update, gathered)


def solution(mesh):
    flat = Mesh(mesh.devices.reshape(2 * CHIPS), ("i",))
    return jax.shard_map(
        on_device,
        mesh=flat,
        in_specs=(P("i", None, None), P("i", None), P("i", None), P("i", None), P("i")),
        out_specs=(P("i", None), P("i", None), P("i", None), P("i", None), P()),
        check_vma=False,
    )
```

```python
import functools

import jax
import jax.numpy as jnp
import numpy as np
from jax import lax
from jax.experimental import pallas as pl
from jax.experimental.pallas import tpu as pltpu
from jax.sharding import Mesh
from jax.sharding import PartitionSpec as P


decay_first = 0.9
decay_second = 0.999
epsilon = 1e-06
weight_decay = 0.01
step_size = 0.05


ROWS = 24
COLS = 512
CHIPS = 64
GROUP = 8
F32 = jnp.float32
BF16 = jnp.bfloat16

NUMBER = np.arange(2 * CHIPS).reshape(2, 2, 4, 4, 2)
PLACE = NUMBER.transpose(3, 2, 4, 0, 1).reshape(4, 4, 4, 2)

CORE_SWAP = [(int(a), int(b)) for pair in PLACE.reshape(CHIPS, 2) for a, b in (pair, pair[::-1])]


def grouping():
    grid = np.zeros((2, GROUP, GROUP), int)
    for core in range(2):
        for a in range(GROUP):
            for b in range(GROUP):
                x, low, z, high = (a >> 1, a & 1, b >> 1, b & 1) if core == 0 else (b >> 1, b & 1, a >> 1, a & 1)
                grid[core, a, b] = PLACE[x, 2 * high + (low ^ high), z, core]
    wide = [grid[core, :, b].tolist() for core in range(2) for b in range(GROUP)]
    narrow = [grid[core, a, :].tolist() for core in range(2) for a in range(GROUP)]
    return wide, narrow


WIDE, NARROW = grouping()


def place_of(device):
    return device >> 6, (device >> 5) & 1, (device >> 3) & 3, (device >> 1) & 3, device & 1


def wide_place(device):
    z_lo, core, y, x, z_hi = place_of(device)
    return jnp.where(core == 0, 2 * x + ((y ^ (y >> 1)) & 1), 2 * (2 * z_hi + z_lo) + (y >> 1))


OFFSETS = ((2, 1), (3, 1), (1, 1), (2, 0), (0, 1), (3, 0), (1, 0))
OWN = (0, 0)
HALVES = (OFFSETS[:4], OFFSETS[4:] + (OWN,))


def source_place(a, offset):
    ring, pair = offset
    return ((((a >> 1) + 4 - ring) & 3) << 1) + ((a & 1) ^ pair)


def target_place(a, offset):
    ring, pair = offset
    return ((((a >> 1) + ring) & 3) << 1) + ((a & 1) ^ pair)


def wide_shift(offset):
    return [(group[source_place(a, offset)], group[a]) for group in WIDE for a in range(GROUP)]


def owner_of(core, a, b):
    first = core == 0
    p = jnp.where(first, a, b)
    q = jnp.where(first, b, a)
    x, z = p >> 1, q >> 1
    y = 2 * (q & 1) + ((p ^ q) & 1)
    return ((z & 1) << 6) + (core << 5) + (y << 3) + (x << 1) + (z >> 1)


def exchange(value, groups):
    return lax.all_to_all(value, "i", 0, 0, axis_index_groups=groups, tiled=True)


def lane_index(rows):
    return lax.broadcasted_iota(jnp.int32, (rows, 128), 1)


def before_kernel(weights, ids, tensor, sums):
    row = lax.broadcasted_iota(jnp.int32, (ROWS, 128), 0)
    of_row = jnp.zeros((ROWS, 128), jnp.int32)
    for k in range(ROWS):
        of_row = jnp.where(row == k, ids[k], of_row)
    tensor[...] = of_row
    lane = lane_index(ROWS)
    kind = lane // 4
    w = weights[...]
    w_sq = jnp.sum(w * w, axis=1, keepdims=True)
    by_kind = jnp.where(kind == 0, w_sq, jnp.where(kind == 2, float(COLS), 0.0))
    per_tensor = jnp.sum(jnp.where(of_row == lane % 4, by_kind, 0.0), axis=0, keepdims=True)
    sums[...] = jnp.broadcast_to(per_tensor, (8, 128))


def update_kernel(parts, weights, first, second, tensor, base, new_first, new_second, update, sums):
    summed = parts[0].astype(F32)
    for k in range(1, GROUP):
        summed = summed + parts[k].astype(F32)
    m = decay_first * first[...] + (1.0 - decay_first) * summed
    v = decay_second * second[...] + (1.0 - decay_second) * summed * summed
    u = m / (jnp.sqrt(v) + epsilon) + weight_decay * weights[...]
    new_first[...] = m
    new_second[...] = v
    update[...] = u
    u_sq = jnp.sum(u * u, axis=1, keepdims=True)
    here = tensor[...] + 4 == lane_index(ROWS)
    per_tensor = jnp.sum(jnp.where(here, u_sq, 0.0), axis=0, keepdims=True)
    sums[...] = base[...] + jnp.broadcast_to(per_tensor, (8, 128))


PAY = 2 * ROWS + 8


def pay_kernel(update, weights, sums, pay):
    total = sums[0, 0:1, :]
    for k in range(1, GROUP):
        total = total + sums[k, 0:1, :]
    high = total.astype(BF16)
    rest = total - high.astype(F32)
    mid = rest.astype(BF16)
    low = (rest - mid.astype(F32)).astype(BF16)
    row = lax.broadcasted_iota(jnp.int32, (8, 128), 0)
    three = jnp.where(
        row == 0, high.astype(F32), jnp.where(row == 1, mid.astype(F32), jnp.where(row == 2, low.astype(F32), 0.0))
    )
    three = jnp.concatenate([three, jnp.zeros((8, COLS - 128), F32)], axis=1)
    one = jnp.concatenate([update[...], weights[...], three], axis=0).astype(BF16)
    for k in range(GROUP):
        pay[k] = one


def trust_and_runs(got):
    total = jnp.zeros((1, 128), F32)
    for k in range(GROUP):
        three = got[k, 2 * ROWS :, 0:128].astype(F32)
        total = total + ((three[0:1] + three[1:2]) + three[2:3])
    update_sq = pltpu.roll(total, 124, 1)
    count = pltpu.roll(total, 120, 1)
    lane = lane_index(1)
    used = lane < 4
    trust = jnp.where(used, jnp.sqrt(total / (update_sq + count)), 0.0)
    rows = jnp.where(used, count * (1.0 / COLS), 0.0)
    start = jnp.zeros((1, 128), F32)
    for k in range(1, 4):
        start = start + jnp.where(lane >= k, pltpu.roll(rows, k, 1), 0.0)
    return trust, start, jnp.where(used, start + rows, -1.0)


def row_trust(first_row, trust, start, end):
    row = (lax.broadcasted_iota(jnp.int32, (ROWS, 128), 0) + first_row).astype(F32)
    here = jnp.logical_and(row >= start, row < end)
    return jnp.sum(jnp.where(here, trust, 0.0), axis=1, keepdims=True)


def params_kernel(me, got, update, weights, params, new_master, scaled_update):
    trust, start, end = trust_and_runs(got)
    core = (me[0] >> 5) & 1
    place = wide_place(me[0])
    for b in range(GROUP):
        factor = row_trust(owner_of(core, place, b) * ROWS, trust, start, end)
        block = got[b, ROWS : 2 * ROWS].astype(F32) - step_size * (factor * got[b, 0:ROWS].astype(F32))
        params[b] = block.astype(BF16)
    scaled = row_trust(me[0] * ROWS, trust, start, end) * update[...]
    scaled_update[...] = scaled
    new_master[...] = weights[...] - step_size * scaled


def take_kernel(me, gradients, *refs, other):
    halves, done = refs[:2], refs[2]
    device = me[0] ^ (32 if other else 0)
    core = (device >> 5) & 1
    for k, offsets in enumerate(HALVES):
        for j, offset in enumerate(offsets):
            a = target_place(wide_place(device), offset)
            for b in range(GROUP):
                pltpu.make_async_copy(gradients.at[owner_of(core, a, b)], halves[k].at[j, b], done.at[k]).start()
    for k in range(2):
        pltpu.make_async_copy(halves[k], halves[k], done.at[k]).wait()


def add_kernel(kept, arrived, *both):
    for j, out in enumerate(both):
        out[...] = kept[j] + arrived[j]


def total_kernel(*refs):
    for b in range(GROUP):
        summed = refs[0][b].astype(F32)
        for part in refs[1:-1]:
            summed = summed + part[b].astype(F32)
        refs[-1][b] = summed.astype(BF16)


def chip_sums_kernel(sums, arrived, out):
    both = sums[...] + arrived[...]
    for k in range(GROUP):
        out[k] = both


def join_kernel(*refs):
    for k, part in enumerate(refs[:-1]):
        refs[-1][k] = part[...]


def place_kernel(me, *refs, arrays, chunks, rows=0):
    blocks, whole = refs[:arrays], refs[arrays : arrays + rows]
    scratch = 1 + (rows > 0)
    outs = refs[len(refs) - scratch - 1 - rows : len(refs) - scratch]
    out, done = outs[0], refs[len(refs) - scratch]
    copies = [pltpu.make_async_copy(whole[k], outs[1 + k], refs[-1].at[k]) for k in range(rows)]
    for array, index, other, offset in chunks:
        device = me[0] ^ (32 if other else 0)
        core = (device >> 5) & 1
        a = source_place(wide_place(device), offset)
        part = blocks[array] if index is None else blocks[array].at[index]
        for b in range(GROUP):
            pltpu.make_async_copy(part.at[b], out.at[owner_of(core, a, b)], done).start()
    for copy in copies:
        copy.start()
    total = len(chunks) * GROUP
    pltpu.make_async_copy(out.at[pl.ds(0, total)], out.at[pl.ds(0, total)], done).wait()
    for copy in copies:
        copy.wait()


SMEM = pl.BlockSpec(memory_space=pltpu.SMEM)
VMEM = pl.BlockSpec(memory_space=pltpu.VMEM)
HBM = pl.BlockSpec(memory_space=pltpu.HBM)


def of(shape, dtype):
    return jax.ShapeDtypeStruct(shape, dtype)


def kernel(body, ins, outs, shapes, limit=8, **more):
    return pl.pallas_call(
        body,
        out_shape=shapes,
        in_specs=ins,
        out_specs=outs,
        compiler_params=pltpu.CompilerParams(vmem_limit_bytes=limit * 2**20),
        **more,
    )


def on_device(gradients, master_weights, first_moment, second_moment, tensor_ids):
    me = lax.axis_index("i").astype(jnp.int32).reshape(1)
    own_f32 = pltpu.VMEM((ROWS, COLS), F32)
    chunk = pltpu.VMEM((GROUP, ROWS, COLS), BF16)

    def send(value, pairs):
        return lax.ppermute(value, "i", pairs)

    blocks = pltpu.with_memory_space_constraint(gradients.reshape(2 * CHIPS, ROWS, COLS), pltpu.HBM)
    half = pltpu.VMEM((4, GROUP, ROWS, COLS), BF16)

    def take(other):
        body = functools.partial(take_kernel, other=other)
        return kernel(
            body, [SMEM, HBM], [VMEM] * 2, [half] * 2, scratch_shapes=[pltpu.SemaphoreType.DMA((2,))]
        )(me, blocks)

    sent = take(True)
    arrived = [send(sent[k], CORE_SWAP) for k in range(2)]
    kept = take(False)
    chunks = []
    for k in range(2):
        chunks += kernel(add_kernel, [VMEM] * 2, [VMEM] * 4, [chunk] * 4)(kept[k], arrived[k])
    tensor, sums = kernel(
        before_kernel, [VMEM, SMEM], (VMEM, VMEM), (pltpu.VMEM((ROWS, 128), jnp.int32), pltpu.VMEM((8, 128), F32))
    )(master_weights, tensor_ids)
    wide = [send(chunks[k], wide_shift(offset)) for k, offset in enumerate(OFFSETS)]
    total = kernel(total_kernel, [VMEM] * 8, VMEM, chunk)(chunks[7], *wide)
    parts = exchange(total, NARROW)

    new_first, new_second, update, sums = kernel(
        update_kernel, [VMEM] * 6, (VMEM,) * 4, (own_f32, own_f32, own_f32, pltpu.VMEM((8, 128), F32))
    )(parts, master_weights, first_moment, second_moment, tensor, sums)

    arrived = lax.ppermute(sums, "i", CORE_SWAP)
    sums = kernel(chip_sums_kernel, [VMEM] * 2, VMEM, pltpu.VMEM((GROUP, 8, 128), F32))(sums, arrived)
    sums = exchange(sums, WIDE)
    pay = kernel(pay_kernel, [VMEM] * 3, VMEM, pltpu.VMEM((GROUP, PAY, COLS), BF16))(update, master_weights, sums)
    got = exchange(pay, NARROW)

    params, new_master, scaled_update = kernel(
        params_kernel, [SMEM] + [VMEM] * 3, (VMEM,) * 3, (chunk, own_f32, own_f32)
    )(me, got, update, master_weights)
    join = lambda *parts: kernel(
        join_kernel, [VMEM] * len(parts), VMEM, pltpu.VMEM((len(parts), GROUP, ROWS, COLS), BF16)
    )(*parts)
    every = of((2 * CHIPS, ROWS, COLS), BF16)

    def place(arrays, chunks, before=None, rows=()):
        first = before is None
        count = len(arrays) + len(rows)
        return kernel(
            functools.partial(place_kernel, arrays=len(arrays), chunks=chunks, rows=len(rows)),
            [SMEM] + [VMEM] * count + ([] if first else [HBM]),
            [HBM] * (1 + len(rows)),
            [every] + [of((ROWS, COLS), F32)] * len(rows),
            input_output_aliases={} if first else {1 + count: 0},
            scratch_shapes=[pltpu.SemaphoreType.DMA] + ([pltpu.SemaphoreType.DMA((len(rows),))] if rows else []),
        )(me, *arrays, *rows, *(() if first else (before,)))

    wide = [send(params, wide_shift(offset)) for offset in OFFSETS]
    other_0 = send(join(params, *wide[0:3]), CORE_SWAP)
    other_1 = send(join(*wide[3:5]), CORE_SWAP)
    other_2 = send(join(*wide[5:7]), CORE_SWAP)
    gathered, new_first, new_second, new_master, scaled_update = place(
        [params, *wide[0:3]],
        [(0, None, False, OWN)] + [(1 + k, None, False, OFFSETS[k]) for k in range(3)],
        rows=(new_first, new_second, new_master, scaled_update),
    )
    (gathered,) = place(
        [*wide[3:7], other_0],
        [(k, None, False, OFFSETS[3 + k]) for k in range(4)]
        + [(4, 0, True, OWN)]
        + [(4, 1 + k, True, OFFSETS[k]) for k in range(3)],
        gathered,
    )
    (gathered,) = place(
        [other_1, other_2],
        [(0, k, True, OFFSETS[3 + k]) for k in range(2)] + [(1, k, True, OFFSETS[5 + k]) for k in range(2)],
        gathered,
    )
    gathered = gathered.reshape(2 * CHIPS * ROWS, COLS)
    return (new_master, new_first, new_second, scaled_update, gathered)


def solution(mesh):
    flat = Mesh(mesh.devices.reshape(2 * CHIPS), ("i",))
    return jax.shard_map(
        on_device,
        mesh=flat,
        in_specs=(P("i", None, None), P("i", None), P("i", None), P("i", None), P("i")),
        out_specs=(P("i", None), P("i", None), P("i", None), P("i", None), P()),
        check_vma=False,
    )
```

```python
import functools

import jax
import jax.numpy as jnp
import numpy as np
from jax import lax
from jax.experimental import pallas as pl
from jax.experimental.pallas import tpu as pltpu
from jax.sharding import Mesh
from jax.sharding import PartitionSpec as P


decay_first = 0.9
decay_second = 0.999
epsilon = 1e-06
weight_decay = 0.01
step_size = 0.05


ROWS = 24
COLS = 512
CHIPS = 64
GROUP = 8
F32 = jnp.float32
BF16 = jnp.bfloat16

NUMBER = np.arange(2 * CHIPS).reshape(2, 2, 4, 4, 2)
PLACE = NUMBER.transpose(3, 2, 4, 0, 1).reshape(4, 4, 4, 2)

CORE_SWAP = [(int(a), int(b)) for pair in PLACE.reshape(CHIPS, 2) for a, b in (pair, pair[::-1])]


def grouping():
    grid = np.zeros((2, GROUP, GROUP), int)
    for core in range(2):
        for a in range(GROUP):
            for b in range(GROUP):
                x, low, z, high = (a >> 1, a & 1, b >> 1, b & 1) if core == 0 else (b >> 1, b & 1, a >> 1, a & 1)
                grid[core, a, b] = PLACE[x, 2 * high + (low ^ high), z, core]
    wide = [grid[core, :, b].tolist() for core in range(2) for b in range(GROUP)]
    narrow = [grid[core, a, :].tolist() for core in range(2) for a in range(GROUP)]
    return wide, narrow


WIDE, NARROW = grouping()


def place_of(device):
    return device >> 6, (device >> 5) & 1, (device >> 3) & 3, (device >> 1) & 3, device & 1


def wide_place(device):
    z_lo, core, y, x, z_hi = place_of(device)
    return jnp.where(core == 0, 2 * x + ((y ^ (y >> 1)) & 1), 2 * (2 * z_hi + z_lo) + (y >> 1))


OFFSETS = ((2, 1), (3, 1), (1, 1), (2, 0), (0, 1), (3, 0), (1, 0))
OWN = (0, 0)
HALVES = (OFFSETS[:4], OFFSETS[4:] + (OWN,))


def source_place(a, offset):
    ring, pair = offset
    return ((((a >> 1) + 4 - ring) & 3) << 1) + ((a & 1) ^ pair)


def target_place(a, offset):
    ring, pair = offset
    return ((((a >> 1) + ring) & 3) << 1) + ((a & 1) ^ pair)


def wide_shift(offset):
    return [(group[source_place(a, offset)], group[a]) for group in WIDE for a in range(GROUP)]


def owner_of(core, a, b):
    first = core == 0
    p = jnp.where(first, a, b)
    q = jnp.where(first, b, a)
    x, z = p >> 1, q >> 1
    y = 2 * (q & 1) + ((p ^ q) & 1)
    return ((z & 1) << 6) + (core << 5) + (y << 3) + (x << 1) + (z >> 1)


def exchange(value, groups):
    return lax.all_to_all(value, "i", 0, 0, axis_index_groups=groups, tiled=True)


def lane_index(rows):
    return lax.broadcasted_iota(jnp.int32, (rows, 128), 1)


def before_kernel(weights, ids, tensor, sums):
    row = lax.broadcasted_iota(jnp.int32, (ROWS, 128), 0)
    of_row = jnp.zeros((ROWS, 128), jnp.int32)
    for k in range(ROWS):
        of_row = jnp.where(row == k, ids[k], of_row)
    tensor[...] = of_row
    lane = lane_index(ROWS)
    kind = lane // 4
    w = weights[...]
    w_sq = jnp.sum(w * w, axis=1, keepdims=True)
    by_kind = jnp.where(kind == 0, w_sq, jnp.where(kind == 2, float(COLS), 0.0))
    per_tensor = jnp.sum(jnp.where(of_row == lane % 4, by_kind, 0.0), axis=0, keepdims=True)
    sums[...] = jnp.broadcast_to(per_tensor, (8, 128))


def update_kernel(parts, weights, first, second, tensor, base, new_first, new_second, update, sums):
    summed = parts[0].astype(F32)
    for k in range(1, GROUP):
        summed = summed + parts[k].astype(F32)
    m = decay_first * first[...] + (1.0 - decay_first) * summed
    v = decay_second * second[...] + (1.0 - decay_second) * summed * summed
    u = m / (jnp.sqrt(v) + epsilon) + weight_decay * weights[...]
    new_first[...] = m
    new_second[...] = v
    update[...] = u
    u_sq = jnp.sum(u * u, axis=1, keepdims=True)
    here = tensor[...] + 4 == lane_index(ROWS)
    per_tensor = jnp.sum(jnp.where(here, u_sq, 0.0), axis=0, keepdims=True)
    sums[...] = base[...] + jnp.broadcast_to(per_tensor, (8, 128))


PAY = 2 * ROWS + 8


def pay_kernel(update, weights, sums, pay):
    total = sums[0, 0:1, :]
    for k in range(1, GROUP):
        total = total + sums[k, 0:1, :]
    high = total.astype(BF16)
    rest = total - high.astype(F32)
    mid = rest.astype(BF16)
    low = (rest - mid.astype(F32)).astype(BF16)
    row = lax.broadcasted_iota(jnp.int32, (8, 128), 0)
    three = jnp.where(
        row == 0, high.astype(F32), jnp.where(row == 1, mid.astype(F32), jnp.where(row == 2, low.astype(F32), 0.0))
    )
    three = jnp.concatenate([three, jnp.zeros((8, COLS - 128), F32)], axis=1)
    one = jnp.concatenate([update[...], weights[...], three], axis=0).astype(BF16)
    for k in range(GROUP):
        pay[k] = one


def trust_and_runs(got):
    total = jnp.zeros((1, 128), F32)
    for k in range(GROUP):
        three = got[k, 2 * ROWS :, 0:128].astype(F32)
        total = total + ((three[0:1] + three[1:2]) + three[2:3])
    update_sq = pltpu.roll(total, 124, 1)
    count = pltpu.roll(total, 120, 1)
    lane = lane_index(1)
    used = lane < 4
    trust = jnp.where(used, jnp.sqrt(total / (update_sq + count)), 0.0)
    rows = jnp.where(used, count * (1.0 / COLS), 0.0)
    start = jnp.zeros((1, 128), F32)
    for k in range(1, 4):
        start = start + jnp.where(lane >= k, pltpu.roll(rows, k, 1), 0.0)
    return trust, start, jnp.where(used, start + rows, -1.0)


def row_trust(first_row, trust, start, end):
    row = (lax.broadcasted_iota(jnp.int32, (ROWS, 128), 0) + first_row).astype(F32)
    here = jnp.logical_and(row >= start, row < end)
    return jnp.sum(jnp.where(here, trust, 0.0), axis=1, keepdims=True)


def params_kernel(me, got, update, weights, params, new_master, scaled_update):
    trust, start, end = trust_and_runs(got)
    core = (me[0] >> 5) & 1
    place = wide_place(me[0])
    for b in range(GROUP):
        factor = row_trust(owner_of(core, place, b) * ROWS, trust, start, end)
        block = got[b, ROWS : 2 * ROWS].astype(F32) - step_size * (factor * got[b, 0:ROWS].astype(F32))
        params[b] = block.astype(BF16)
    scaled = row_trust(me[0] * ROWS, trust, start, end) * update[...]
    scaled_update[...] = scaled
    new_master[...] = weights[...] - step_size * scaled


def take_kernel(me, gradients, *refs, other):
    halves, done = refs[:2], refs[2]
    device = me[0] ^ (32 if other else 0)
    core = (device >> 5) & 1
    for k, offsets in enumerate(HALVES):
        for j, offset in enumerate(offsets):
            a = target_place(wide_place(device), offset)
            for b in range(GROUP):
                pltpu.make_async_copy(gradients.at[owner_of(core, a, b)], halves[k].at[j, b], done.at[k]).start()
    for k in range(2):
        pltpu.make_async_copy(halves[k], halves[k], done.at[k]).wait()


def add_kernel(kept, arrived, *both):
    for j, out in enumerate(both):
        out[...] = kept[j] + arrived[j]


def total_kernel(*refs):
    for b in range(GROUP):
        summed = refs[0][b].astype(F32)
        for part in refs[1:-1]:
            summed = summed + part[b].astype(F32)
        refs[-1][b] = summed.astype(BF16)


def chip_sums_kernel(sums, arrived, out):
    both = sums[...] + arrived[...]
    for k in range(GROUP):
        out[k] = both


def join_kernel(*refs):
    for k, part in enumerate(refs[:-1]):
        refs[-1][k] = part[...]


def place_kernel(me, *refs, arrays, chunks, rows=0):
    blocks, whole = refs[:arrays], refs[arrays : arrays + rows]
    scratch = 1 + (rows > 0)
    outs = refs[len(refs) - scratch - 1 - rows : len(refs) - scratch]
    out, done = outs[0], refs[len(refs) - scratch]
    copies = [pltpu.make_async_copy(whole[k], outs[1 + k], refs[-1].at[k]) for k in range(rows)]
    for array, index, other, offset in chunks:
        device = me[0] ^ (32 if other else 0)
        core = (device >> 5) & 1
        a = source_place(wide_place(device), offset)
        part = blocks[array] if index is None else blocks[array].at[index]
        for b in range(GROUP):
            pltpu.make_async_copy(part.at[b], out.at[owner_of(core, a, b)], done).start()
    for copy in copies:
        copy.start()
    total = len(chunks) * GROUP
    pltpu.make_async_copy(out.at[pl.ds(0, total)], out.at[pl.ds(0, total)], done).wait()
    for copy in copies:
        copy.wait()


SMEM = pl.BlockSpec(memory_space=pltpu.SMEM)
VMEM = pl.BlockSpec(memory_space=pltpu.VMEM)
HBM = pl.BlockSpec(memory_space=pltpu.HBM)


def of(shape, dtype):
    return jax.ShapeDtypeStruct(shape, dtype)


def kernel(body, ins, outs, shapes, limit=8, **more):
    return pl.pallas_call(
        body,
        out_shape=shapes,
        in_specs=ins,
        out_specs=outs,
        compiler_params=pltpu.CompilerParams(vmem_limit_bytes=limit * 2**20),
        **more,
    )


def on_device(gradients, master_weights, first_moment, second_moment, tensor_ids):
    me = lax.axis_index("i").astype(jnp.int32).reshape(1)
    own_f32 = pltpu.VMEM((ROWS, COLS), F32)
    chunk = pltpu.VMEM((GROUP, ROWS, COLS), BF16)

    def send(value, pairs):
        return lax.ppermute(value, "i", pairs)

    blocks = pltpu.with_memory_space_constraint(gradients.reshape(2 * CHIPS, ROWS, COLS), pltpu.HBM)
    half = pltpu.VMEM((4, GROUP, ROWS, COLS), BF16)

    def take(other):
        body = functools.partial(take_kernel, other=other)
        return kernel(
            body, [SMEM, HBM], [VMEM] * 2, [half] * 2, scratch_shapes=[pltpu.SemaphoreType.DMA((2,))]
        )(me, blocks)

    sent = take(True)
    arrived = [send(sent[k], CORE_SWAP) for k in range(2)]
    kept = take(False)
    chunks = []
    for k in range(2):
        chunks += kernel(add_kernel, [VMEM] * 2, [VMEM] * 4, [chunk] * 4)(kept[k], arrived[k])
    tensor, sums = kernel(
        before_kernel, [VMEM, SMEM], (VMEM, VMEM), (pltpu.VMEM((ROWS, 128), jnp.int32), pltpu.VMEM((8, 128), F32))
    )(master_weights, tensor_ids)
    wide = [send(chunks[k], wide_shift(offset)) for k, offset in enumerate(OFFSETS)]
    total = kernel(total_kernel, [VMEM] * 8, VMEM, chunk)(chunks[7], *wide)
    parts = exchange(total, NARROW)

    new_first, new_second, update, sums = kernel(
        update_kernel, [VMEM] * 6, (VMEM,) * 4, (own_f32, own_f32, own_f32, pltpu.VMEM((8, 128), F32))
    )(parts, master_weights, first_moment, second_moment, tensor, sums)

    arrived = lax.ppermute(sums, "i", CORE_SWAP)
    sums = kernel(chip_sums_kernel, [VMEM] * 2, VMEM, pltpu.VMEM((GROUP, 8, 128), F32))(sums, arrived)
    sums = exchange(sums, WIDE)
    pay = kernel(pay_kernel, [VMEM] * 3, VMEM, pltpu.VMEM((GROUP, PAY, COLS), BF16))(update, master_weights, sums)
    got = exchange(pay, NARROW)

    params, new_master, scaled_update = kernel(
        params_kernel, [SMEM] + [VMEM] * 3, (VMEM,) * 3, (chunk, own_f32, own_f32)
    )(me, got, update, master_weights)
    join = lambda *parts: kernel(
        join_kernel, [VMEM] * len(parts), VMEM, pltpu.VMEM((len(parts), GROUP, ROWS, COLS), BF16)
    )(*parts)
    every = of((2 * CHIPS, ROWS, COLS), BF16)

    def place(arrays, chunks, before=None, rows=()):
        first = before is None
        count = len(arrays) + len(rows)
        return kernel(
            functools.partial(place_kernel, arrays=len(arrays), chunks=chunks, rows=len(rows)),
            [SMEM] + [VMEM] * count + ([] if first else [HBM]),
            [HBM] * (1 + len(rows)),
            [every] + [of((ROWS, COLS), F32)] * len(rows),
            input_output_aliases={} if first else {1 + count: 0},
            scratch_shapes=[pltpu.SemaphoreType.DMA] + ([pltpu.SemaphoreType.DMA((len(rows),))] if rows else []),
        )(me, *arrays, *rows, *(() if first else (before,)))

    wide = [send(params, wide_shift(offset)) for offset in OFFSETS]
    split = 4
    other_0 = send(join(params, *wide[:split]), CORE_SWAP)
    other_1 = send(join(*wide[split:]), CORE_SWAP)
    gathered, new_first, new_second, new_master, scaled_update = place(
        [params], [(0, None, False, OWN)], rows=(new_first, new_second, new_master, scaled_update)
    )
    (gathered,) = place(
        [*wide, other_0],
        [(k, None, False, offset) for k, offset in enumerate(OFFSETS)]
        + [(7, k, True, offset) for k, offset in enumerate((OWN,) + OFFSETS[:split])],
        gathered,
    )
    (gathered,) = place([other_1], [(0, k, True, offset) for k, offset in enumerate(OFFSETS[split:])], gathered)
    gathered = gathered.reshape(2 * CHIPS * ROWS, COLS)
    return (new_master, new_first, new_second, scaled_update, gathered)


def solution(mesh):
    flat = Mesh(mesh.devices.reshape(2 * CHIPS), ("i",))
    return jax.shard_map(
        on_device,
        mesh=flat,
        in_specs=(P("i", None, None), P("i", None), P("i", None), P("i", None), P("i")),
        out_specs=(P("i", None), P("i", None), P("i", None), P("i", None), P()),
        check_vma=False,
    )
```

```python
import functools

import jax
import jax.numpy as jnp
import numpy as np
from jax import lax
from jax.experimental import pallas as pl
from jax.experimental.pallas import tpu as pltpu
from jax.sharding import Mesh
from jax.sharding import PartitionSpec as P


decay_first = 0.9
decay_second = 0.999
epsilon = 1e-06
weight_decay = 0.01
step_size = 0.05


ROWS = 24
COLS = 512
CHIPS = 64
GROUP = 8
F32 = jnp.float32
BF16 = jnp.bfloat16

NUMBER = np.arange(2 * CHIPS).reshape(2, 2, 4, 4, 2)
PLACE = NUMBER.transpose(3, 2, 4, 0, 1).reshape(4, 4, 4, 2)

CORE_SWAP = [(int(a), int(b)) for pair in PLACE.reshape(CHIPS, 2) for a, b in (pair, pair[::-1])]


def grouping():
    grid = np.zeros((2, GROUP, GROUP), int)
    for core in range(2):
        for a in range(GROUP):
            for b in range(GROUP):
                x, low, z, high = (a >> 1, a & 1, b >> 1, b & 1) if core == 0 else (b >> 1, b & 1, a >> 1, a & 1)
                grid[core, a, b] = PLACE[x, 2 * high + (low ^ high), z, core]
    wide = [grid[core, :, b].tolist() for core in range(2) for b in range(GROUP)]
    narrow = [grid[core, a, :].tolist() for core in range(2) for a in range(GROUP)]
    return wide, narrow


WIDE, NARROW = grouping()


def place_of(device):
    return device >> 6, (device >> 5) & 1, (device >> 3) & 3, (device >> 1) & 3, device & 1


def group_places(device):
    z_lo, core, y, x, z_hi = place_of(device)
    p = 2 * x + ((y ^ (y >> 1)) & 1)
    q = 2 * (2 * z_hi + z_lo) + (y >> 1)
    return jnp.where(core == 0, p, q), jnp.where(core == 0, q, p)


OFFSETS = ((2, 1), (3, 1), (1, 1), (2, 0), (0, 1), (3, 0), (1, 0))
OWN = (0, 0)
HALVES = (OFFSETS[:4], OFFSETS[4:] + (OWN,))
RINGS = (0, 2, 3, 1)


def source_place(a, offset):
    ring, pair = offset
    return ((((a >> 1) + 4 - ring) & 3) << 1) + ((a & 1) ^ pair)


def target_place(a, offset):
    ring, pair = offset
    return ((((a >> 1) + ring) & 3) << 1) + ((a & 1) ^ pair)


def shift(groups, offset):
    return [(group[source_place(a, offset)], group[a]) for group in groups for a in range(GROUP)]


def owner_of(core, a, b):
    first = core == 0
    p = jnp.where(first, a, b)
    q = jnp.where(first, b, a)
    x, z = p >> 1, q >> 1
    y = 2 * (q & 1) + ((p ^ q) & 1)
    return ((z & 1) << 6) + (core << 5) + (y << 3) + (x << 1) + (z >> 1)


def exchange(value, groups):
    return lax.all_to_all(value, "i", 0, 0, axis_index_groups=groups, tiled=True)


def lane_index(rows):
    return lax.broadcasted_iota(jnp.int32, (rows, 128), 1)


def before_kernel(weights, ids, tensor, sums):
    row = lax.broadcasted_iota(jnp.int32, (ROWS, 128), 0)
    of_row = jnp.zeros((ROWS, 128), jnp.int32)
    for k in range(ROWS):
        of_row = jnp.where(row == k, ids[k], of_row)
    tensor[...] = of_row
    lane = lane_index(ROWS)
    kind = lane // 4
    w = weights[...]
    w_sq = jnp.sum(w * w, axis=1, keepdims=True)
    by_kind = jnp.where(kind == 0, w_sq, jnp.where(kind == 2, float(COLS), 0.0))
    per_tensor = jnp.sum(jnp.where(of_row == lane % 4, by_kind, 0.0), axis=0, keepdims=True)
    sums[...] = jnp.broadcast_to(per_tensor, (8, 128))


def update_kernel(parts, weights, first, second, tensor, base, new_first, new_second, update, sums):
    summed = parts[0].astype(F32)
    for k in range(1, GROUP):
        summed = summed + parts[k].astype(F32)
    m = decay_first * first[...] + (1.0 - decay_first) * summed
    v = decay_second * second[...] + (1.0 - decay_second) * summed * summed
    u = m / (jnp.sqrt(v) + epsilon) + weight_decay * weights[...]
    new_first[...] = m
    new_second[...] = v
    update[...] = u
    u_sq = jnp.sum(u * u, axis=1, keepdims=True)
    here = tensor[...] + 4 == lane_index(ROWS)
    per_tensor = jnp.sum(jnp.where(here, u_sq, 0.0), axis=0, keepdims=True)
    sums[...] = base[...] + jnp.broadcast_to(per_tensor, (8, 128))


PAY = ROWS + 8


def in_three(total):
    high = total.astype(BF16).astype(F32)
    rest = total - high
    mid = rest.astype(BF16).astype(F32)
    low = (rest - mid).astype(BF16).astype(F32)
    row = lax.broadcasted_iota(jnp.int32, (8, 128), 0)
    three = jnp.where(row == 0, high, jnp.where(row == 1, mid, jnp.where(row == 2, low, 0.0)))
    return jnp.concatenate([three, jnp.zeros((8, COLS - 128), F32)], axis=1)


def pay_kernel(update, sums, pay):
    one = jnp.concatenate([update[...], in_three(sums[0:1, :])], axis=0).astype(BF16)
    for k in range(GROUP):
        pay[k] = one


def open_kernel(got, updates):
    total = jnp.zeros((1, 128), F32)
    for k in range(GROUP):
        updates[k] = got[k, 0:ROWS]
        three = got[k, ROWS:, 0:128].astype(F32)
        total = total + ((three[0:1] + three[1:2]) + three[2:3])
    updates[GROUP] = jnp.concatenate([in_three(total), jnp.zeros((ROWS - 8, COLS), F32)], axis=0).astype(BF16)


def trust_and_runs(total):
    update_sq = pltpu.roll(total, 124, 1)
    count = pltpu.roll(total, 120, 1)
    lane = lane_index(1)
    used = lane < 4
    trust = jnp.where(used, jnp.sqrt(total / (update_sq + count)), 0.0)
    rows = jnp.where(used, count * (1.0 / COLS), 0.0)
    start = jnp.zeros((1, 128), F32)
    for k in range(1, 4):
        start = start + jnp.where(lane >= k, pltpu.roll(rows, k, 1), 0.0)
    return trust, start, jnp.where(used, start + rows, -1.0)


def row_trust(first_row, trust, start, end):
    row = (lax.broadcasted_iota(jnp.int32, (ROWS, 128), 0) + first_row).astype(F32)
    here = jnp.logical_and(row >= start, row < end)
    return jnp.sum(jnp.where(here, trust, 0.0), axis=1, keepdims=True)


def core_total_kernel(me, *refs):
    parts, (out, totals) = refs[:GROUP], refs[GROUP:]
    place = group_places(me[0])[0]
    for part, offset in zip(parts, OFFSETS + (OWN,)):
        three = part[GROUP, 0:8, 0:128].astype(F32)
        total = (three[0:1] + three[1:2]) + three[2:3]
        totals[source_place(place, offset)] = jnp.broadcast_to(total, (8, 128))
    total = totals[0]
    for k in range(1, GROUP):
        total = total + totals[k]
    out[...] = total


def trust_kernel(me, total, arrived, update, weights, out, new_master, scaled_update):
    three = trust_and_runs(total[0:1, :] + arrived[0:1, :])
    for k in range(3):
        out[k] = jnp.broadcast_to(three[k], (8, 128))
    scaled = row_trust(me[0] * ROWS, *three) * update[...]
    scaled_update[...] = scaled
    new_master[...] = weights[...] - step_size * scaled


def params_kernel(me, trust, *refs, offsets):
    updates, held, params = refs[: len(offsets)], refs[len(offsets) : -1], refs[-1]
    three = trust[0, 0:1, :], trust[1, 0:1, :], trust[2, 0:1, :]
    core = (me[0] >> 5) & 1
    place, place_b = group_places(me[0])
    for ring, weights in zip(RINGS, held):
        for pair in range(2):
            b = source_place(place_b, (ring, pair))
            for j, offset in enumerate(offsets):
                factor = row_trust(owner_of(core, source_place(place, offset), b) * ROWS, *three)
                member = (OFFSETS + (OWN,)).index(offset)
                block = weights[pair, member].astype(F32) - step_size * (factor * updates[j][b].astype(F32))
                params[j, b] = block.astype(BF16)


def take_kernel(me, gradients, *refs, other):
    halves, done = refs[:2], refs[2]
    device = me[0] ^ (32 if other else 0)
    core = (device >> 5) & 1
    for k, offsets in enumerate(HALVES):
        for j, offset in enumerate(offsets):
            a = target_place(group_places(device)[0], offset)
            for b in range(GROUP):
                pltpu.make_async_copy(gradients.at[owner_of(core, a, b)], halves[k].at[j, b], done.at[k]).start()
    for k in range(2):
        pltpu.make_async_copy(halves[k], halves[k], done.at[k]).wait()


def add_kernel(kept, arrived, weights, *both):
    for j, out in enumerate(both):
        out[0:GROUP] = kept[j] + arrived[j]
        out[GROUP] = weights[...].astype(BF16)


def total_kernel(*refs):
    parts, (total, members) = refs[:-2], refs[-2:]
    for b in range(GROUP):
        summed = parts[GROUP - 1][b].astype(F32)
        for part in parts[: GROUP - 1]:
            summed = summed + part[b].astype(F32)
        total[b] = summed.astype(BF16)
    for j, part in enumerate(parts):
        members[j] = part[GROUP]


def join_kernel(*refs):
    for k, part in enumerate(refs[:-1]):
        refs[-1][k] = part[...]


def place_kernel(me, *refs, arrays, chunks, rows=0):
    blocks, whole = refs[:arrays], refs[arrays : arrays + rows]
    scratch = 1 + (rows > 0)
    outs = refs[len(refs) - scratch - 1 - rows : len(refs) - scratch]
    out, done = outs[0], refs[len(refs) - scratch]
    copies = [pltpu.make_async_copy(whole[k], outs[1 + k], refs[-1].at[k]) for k in range(rows)]
    for array, index, other, offset in chunks:
        device = me[0] ^ (32 if other else 0)
        core = (device >> 5) & 1
        a = source_place(group_places(device)[0], offset)
        part = blocks[array] if index is None else blocks[array].at[index]
        for b in range(GROUP):
            pltpu.make_async_copy(part.at[b], out.at[owner_of(core, a, b)], done).start()
    for copy in copies:
        copy.start()
    total = len(chunks) * GROUP
    pltpu.make_async_copy(out.at[pl.ds(0, total)], out.at[pl.ds(0, total)], done).wait()
    for copy in copies:
        copy.wait()


SMEM = pl.BlockSpec(memory_space=pltpu.SMEM)
VMEM = pl.BlockSpec(memory_space=pltpu.VMEM)
HBM = pl.BlockSpec(memory_space=pltpu.HBM)


def of(shape, dtype):
    return jax.ShapeDtypeStruct(shape, dtype)


def kernel(body, ins, outs, shapes, limit=4, **more):
    return pl.pallas_call(
        body,
        out_shape=shapes,
        in_specs=ins,
        out_specs=outs,
        compiler_params=pltpu.CompilerParams(vmem_limit_bytes=limit * 2**20),
        **more,
    )


def on_device(gradients, master_weights, first_moment, second_moment, tensor_ids):
    me = lax.axis_index("i").astype(jnp.int32).reshape(1)
    own_f32 = pltpu.VMEM((ROWS, COLS), F32)
    chunk = pltpu.VMEM((GROUP, ROWS, COLS), BF16)

    def send(value, pairs):
        return lax.ppermute(value, "i", pairs)

    blocks = pltpu.with_memory_space_constraint(gradients.reshape(2 * CHIPS, ROWS, COLS), pltpu.HBM)
    half = pltpu.VMEM((4, GROUP, ROWS, COLS), BF16)

    def take(other):
        body = functools.partial(take_kernel, other=other)
        return kernel(
            body, [SMEM, HBM], [VMEM] * 2, [half] * 2, scratch_shapes=[pltpu.SemaphoreType.DMA((2,))]
        )(me, blocks)

    sent = take(True)
    arrived = [send(sent[k], CORE_SWAP) for k in range(2)]
    kept = take(False)
    chunks = []
    more = pltpu.VMEM((GROUP + 1, ROWS, COLS), BF16)
    for k in range(2):
        chunks += kernel(add_kernel, [VMEM] * 3, [VMEM] * 4, [more] * 4)(kept[k], arrived[k], master_weights)
    tensor, sums = kernel(
        before_kernel, [VMEM, SMEM], (VMEM, VMEM), (pltpu.VMEM((ROWS, 128), jnp.int32), pltpu.VMEM((8, 128), F32))
    )(master_weights, tensor_ids)
    wide = [send(chunks[k], shift(WIDE, offset)) for k, offset in enumerate(OFFSETS)]
    total, members = kernel(total_kernel, [VMEM] * 8, [VMEM] * 2, [chunk] * 2)(*wide, chunks[7])
    parts = exchange(total, NARROW)
    pair = send(members, shift(NARROW, (0, 1)))
    pair = kernel(join_kernel, [VMEM] * 2, VMEM, pltpu.VMEM((2, GROUP, ROWS, COLS), BF16))(members, pair)
    held = [pair] + [send(pair, shift(NARROW, (ring, 0))) for ring in RINGS[1:]]

    new_first, new_second, update, sums = kernel(
        update_kernel, [VMEM] * 6, (VMEM,) * 4, (own_f32, own_f32, own_f32, pltpu.VMEM((8, 128), F32))
    )(parts, master_weights, first_moment, second_moment, tensor, sums)

    pay = kernel(pay_kernel, [VMEM] * 2, VMEM, of((GROUP, PAY, COLS), BF16))(update, sums)
    got = exchange(pay, NARROW)
    updates = kernel(open_kernel, [VMEM], VMEM, more)(got)
    wide = [send(updates, shift(WIDE, offset)) for offset in OFFSETS]
    total = kernel(
        core_total_kernel,
        [SMEM] + [VMEM] * GROUP,
        VMEM,
        pltpu.VMEM((8, 128), F32),
        scratch_shapes=[pltpu.VMEM((GROUP, 8, 128), F32)],
    )(me, *wide, updates)
    arrived = send(total, CORE_SWAP)
    trust, new_master, scaled_update = kernel(
        trust_kernel, [SMEM] + [VMEM] * 4, (VMEM,) * 3, (pltpu.VMEM((3, 8, 128), F32), own_f32, own_f32)
    )(me, total, arrived, update, master_weights)

    def params_of(offsets, values):
        body = functools.partial(params_kernel, offsets=offsets)
        shape = pltpu.VMEM((len(offsets), GROUP, ROWS, COLS), BF16)
        return kernel(body, [SMEM] + [VMEM] * (5 + len(values)), VMEM, shape)(me, trust, *values, *held)

    first, last = (OWN,) + OFFSETS[:3], OFFSETS[3:]
    params_0 = params_of(first, (updates, *wide[:3]))
    params_1 = params_of(last, wide[3:])
    other_0 = send(params_0, CORE_SWAP)
    other_1 = send(params_1, CORE_SWAP)
    every = of((2 * CHIPS, ROWS, COLS), BF16)

    def place(arrays, chunks, before=None, rows=()):
        first = before is None
        count = len(arrays) + len(rows)
        return kernel(
            functools.partial(place_kernel, arrays=len(arrays), chunks=chunks, rows=len(rows)),
            [SMEM] + [VMEM] * count + ([] if first else [HBM]),
            [HBM] * (1 + len(rows)),
            [every] + [of((ROWS, COLS), F32)] * len(rows),
            input_output_aliases={} if first else {1 + count: 0},
            scratch_shapes=[pltpu.SemaphoreType.DMA] + ([pltpu.SemaphoreType.DMA((len(rows),))] if rows else []),
        )(me, *arrays, *rows, *(() if first else (before,)))

    listed = lambda array, other, offsets: [(array, k, other, offset) for k, offset in enumerate(offsets)]
    gathered, new_first, new_second, new_master, scaled_update = place(
        [params_0, params_1],
        listed(0, False, first) + listed(1, False, last),
        rows=(new_first, new_second, new_master, scaled_update),
    )
    (gathered,) = place([other_0], listed(0, True, first), gathered)
    (gathered,) = place([other_1], listed(0, True, last), gathered)
    gathered = gathered.reshape(2 * CHIPS * ROWS, COLS)
    return (new_master, new_first, new_second, scaled_update, gathered)


def solution(mesh):
    flat = Mesh(mesh.devices.reshape(2 * CHIPS), ("i",))
    return jax.shard_map(
        on_device,
        mesh=flat,
        in_specs=(P("i", None, None), P("i", None), P("i", None), P("i", None), P("i")),
        out_specs=(P("i", None), P("i", None), P("i", None), P("i", None), P()),
        check_vma=False,
    )
```

```python
import functools

import jax
import jax.numpy as jnp
import numpy as np
from jax import lax
from jax.experimental import pallas as pl
from jax.experimental.pallas import tpu as pltpu
from jax.sharding import Mesh
from jax.sharding import PartitionSpec as P


decay_first = 0.9
decay_second = 0.999
epsilon = 1e-06
weight_decay = 0.01
step_size = 0.05


ROWS = 24
COLS = 512
CHIPS = 64
GROUP = 8
F32 = jnp.float32
BF16 = jnp.bfloat16

NUMBER = np.arange(2 * CHIPS).reshape(2, 2, 4, 4, 2)
PLACE = NUMBER.transpose(3, 2, 4, 0, 1).reshape(4, 4, 4, 2)

CORE_SWAP = [(int(a), int(b)) for pair in PLACE.reshape(CHIPS, 2) for a, b in (pair, pair[::-1])]


def grouping():
    grid = np.zeros((2, GROUP, GROUP), int)
    for core in range(2):
        for a in range(GROUP):
            for b in range(GROUP):
                x, low, z, high = (a >> 1, a & 1, b >> 1, b & 1) if core == 0 else (b >> 1, b & 1, a >> 1, a & 1)
                grid[core, a, b] = PLACE[x, 2 * high + (low ^ high), z, core]
    wide = [grid[core, :, b].tolist() for core in range(2) for b in range(GROUP)]
    narrow = [grid[core, a, :].tolist() for core in range(2) for a in range(GROUP)]
    return wide, narrow


WIDE, NARROW = grouping()


def place_of(device):
    return device >> 6, (device >> 5) & 1, (device >> 3) & 3, (device >> 1) & 3, device & 1


def group_places(device):
    z_lo, core, y, x, z_hi = place_of(device)
    p = 2 * x + ((y ^ (y >> 1)) & 1)
    q = 2 * (2 * z_hi + z_lo) + (y >> 1)
    return jnp.where(core == 0, p, q), jnp.where(core == 0, q, p)


OFFSETS = ((2, 1), (3, 1), (1, 1), (2, 0), (0, 1), (3, 0), (1, 0))
OWN = (0, 0)
HALVES = (OFFSETS[:4], OFFSETS[4:] + (OWN,))
RINGS = (0, 1, 3, 2)


def source_place(a, offset):
    ring, pair = offset
    return ((((a >> 1) + 4 - ring) & 3) << 1) + ((a & 1) ^ pair)


def target_place(a, offset):
    ring, pair = offset
    return ((((a >> 1) + ring) & 3) << 1) + ((a & 1) ^ pair)


def shift(groups, offset):
    return [(group[source_place(a, offset)], group[a]) for group in groups for a in range(GROUP)]


def owner_of(core, a, b):
    first = core == 0
    p = jnp.where(first, a, b)
    q = jnp.where(first, b, a)
    x, z = p >> 1, q >> 1
    y = 2 * (q & 1) + ((p ^ q) & 1)
    return ((z & 1) << 6) + (core << 5) + (y << 3) + (x << 1) + (z >> 1)


def exchange(value, groups):
    return lax.all_to_all(value, "i", 0, 0, axis_index_groups=groups, tiled=True)


def lane_index(rows):
    return lax.broadcasted_iota(jnp.int32, (rows, 128), 1)


def before_kernel(weights, ids, tensor, sums):
    row = lax.broadcasted_iota(jnp.int32, (ROWS, 128), 0)
    of_row = jnp.zeros((ROWS, 128), jnp.int32)
    for k in range(ROWS):
        of_row = jnp.where(row == k, ids[k], of_row)
    tensor[...] = of_row
    lane = lane_index(ROWS)
    kind = lane // 4
    w = weights[...]
    w_sq = jnp.sum(w * w, axis=1, keepdims=True)
    by_kind = jnp.where(kind == 0, w_sq, jnp.where(kind == 2, float(COLS), 0.0))
    per_tensor = jnp.sum(jnp.where(of_row == lane % 4, by_kind, 0.0), axis=0, keepdims=True)
    sums[...] = jnp.broadcast_to(per_tensor, (8, 128))


def update_kernel(parts, weights, first, second, tensor, base, new_first, new_second, update, sums):
    summed = parts[0].astype(F32)
    for k in range(1, GROUP):
        summed = summed + parts[k].astype(F32)
    m = decay_first * first[...] + (1.0 - decay_first) * summed
    v = decay_second * second[...] + (1.0 - decay_second) * summed * summed
    u = m / (jnp.sqrt(v) + epsilon) + weight_decay * weights[...]
    new_first[...] = m
    new_second[...] = v
    update[...] = u
    u_sq = jnp.sum(u * u, axis=1, keepdims=True)
    here = tensor[...] + 4 == lane_index(ROWS)
    per_tensor = jnp.sum(jnp.where(here, u_sq, 0.0), axis=0, keepdims=True)
    sums[...] = base[...] + jnp.broadcast_to(per_tensor, (8, 128))


PAY = ROWS + 8


def in_three(total):
    high = total.astype(BF16).astype(F32)
    rest = total - high
    mid = rest.astype(BF16).astype(F32)
    low = (rest - mid).astype(BF16).astype(F32)
    row = lax.broadcasted_iota(jnp.int32, (8, 128), 0)
    three = jnp.where(row == 0, high, jnp.where(row == 1, mid, jnp.where(row == 2, low, 0.0)))
    return jnp.concatenate([three, jnp.zeros((8, COLS - 128), F32)], axis=1)


def pay_kernel(update, sums, pay):
    one = jnp.concatenate([update[...], in_three(sums[0:1, :])], axis=0).astype(BF16)
    for k in range(GROUP):
        pay[k] = one


def open_kernel(got, updates):
    total = jnp.zeros((1, 128), F32)
    for k in range(GROUP):
        updates[k] = got[k, 0:ROWS]
        three = got[k, ROWS:, 0:128].astype(F32)
        total = total + ((three[0:1] + three[1:2]) + three[2:3])
    updates[GROUP] = jnp.concatenate([in_three(total), jnp.zeros((ROWS - 8, COLS), F32)], axis=0).astype(BF16)


def trust_and_runs(total):
    update_sq = pltpu.roll(total, 124, 1)
    count = pltpu.roll(total, 120, 1)
    lane = lane_index(1)
    used = lane < 4
    trust = jnp.where(used, jnp.sqrt(total / (update_sq + count)), 0.0)
    rows = jnp.where(used, count * (1.0 / COLS), 0.0)
    start = jnp.zeros((1, 128), F32)
    for k in range(1, 4):
        start = start + jnp.where(lane >= k, pltpu.roll(rows, k, 1), 0.0)
    return trust, start, jnp.where(used, start + rows, -1.0)


def row_trust(first_row, trust, start, end):
    row = (lax.broadcasted_iota(jnp.int32, (ROWS, 128), 0) + first_row).astype(F32)
    here = jnp.logical_and(row >= start, row < end)
    return jnp.sum(jnp.where(here, trust, 0.0), axis=1, keepdims=True)


def core_total_kernel(me, *refs):
    parts, (out, totals) = refs[:GROUP], refs[GROUP:]
    place = group_places(me[0])[0]
    for part, offset in zip(parts, OFFSETS + (OWN,)):
        three = part[GROUP, 0:8, 0:128].astype(F32)
        total = (three[0:1] + three[1:2]) + three[2:3]
        totals[source_place(place, offset)] = jnp.broadcast_to(total, (8, 128))
    total = totals[0]
    for k in range(1, GROUP):
        total = total + totals[k]
    out[...] = total


def trust_kernel(me, total, arrived, update, weights, out, new_master, scaled_update):
    three = trust_and_runs(total[0:1, :] + arrived[0:1, :])
    for k in range(3):
        out[k] = jnp.broadcast_to(three[k], (8, 128))
    scaled = row_trust(me[0] * ROWS, *three) * update[...]
    scaled_update[...] = scaled
    new_master[...] = weights[...] - step_size * scaled


def params_kernel(me, trust, *refs, offsets):
    updates, held, params = refs[: len(offsets)], refs[len(offsets) : -1], refs[-1]
    three = trust[0, 0:1, :], trust[1, 0:1, :], trust[2, 0:1, :]
    core = (me[0] >> 5) & 1
    place, place_b = group_places(me[0])
    for ring, weights in zip(RINGS, held):
        for pair in range(2):
            b = source_place(place_b, (ring, pair))
            for j, offset in enumerate(offsets):
                factor = row_trust(owner_of(core, source_place(place, offset), b) * ROWS, *three)
                member = (OFFSETS + (OWN,)).index(offset)
                block = weights[pair, member].astype(F32) - step_size * (factor * updates[j][b].astype(F32))
                params[j, b] = block.astype(BF16)


def take_kernel(me, gradients, *refs, other):
    halves, done = refs[:2], refs[2]
    device = me[0] ^ (32 if other else 0)
    core = (device >> 5) & 1
    for k, offsets in enumerate(HALVES):
        for j, offset in enumerate(offsets):
            a = target_place(group_places(device)[0], offset)
            for b in range(GROUP):
                pltpu.make_async_copy(gradients.at[owner_of(core, a, b)], halves[k].at[j, b], done.at[k]).start()
    for k in range(2):
        pltpu.make_async_copy(halves[k], halves[k], done.at[k]).wait()


def add_kernel(kept, arrived, weights, *both):
    for j, out in enumerate(both):
        out[0:GROUP] = kept[j] + arrived[j]
        out[GROUP] = weights[...].astype(BF16)


def total_kernel(*refs):
    parts, (total, members) = refs[:-2], refs[-2:]
    for b in range(GROUP):
        summed = parts[GROUP - 1][b].astype(F32)
        for part in parts[: GROUP - 1]:
            summed = summed + part[b].astype(F32)
        total[b] = summed.astype(BF16)
    for j, part in enumerate(parts):
        members[j] = part[GROUP]


def join_kernel(*refs):
    for k, part in enumerate(refs[:-1]):
        refs[-1][k] = part[...]


def place_kernel(me, *refs, arrays, chunks, rows=0):
    blocks, whole = refs[:arrays], refs[arrays : arrays + rows]
    scratch = 1 + (rows > 0)
    outs = refs[len(refs) - scratch - 1 - rows : len(refs) - scratch]
    out, done = outs[0], refs[len(refs) - scratch]
    copies = [pltpu.make_async_copy(whole[k], outs[1 + k], refs[-1].at[k]) for k in range(rows)]
    for array, index, other, offset in chunks:
        device = me[0] ^ (32 if other else 0)
        core = (device >> 5) & 1
        a = source_place(group_places(device)[0], offset)
        part = blocks[array] if index is None else blocks[array].at[index]
        for b in range(GROUP):
            pltpu.make_async_copy(part.at[b], out.at[owner_of(core, a, b)], done).start()
    for copy in copies:
        copy.start()
    total = len(chunks) * GROUP
    pltpu.make_async_copy(out.at[pl.ds(0, total)], out.at[pl.ds(0, total)], done).wait()
    for copy in copies:
        copy.wait()


SMEM = pl.BlockSpec(memory_space=pltpu.SMEM)
VMEM = pl.BlockSpec(memory_space=pltpu.VMEM)
HBM = pl.BlockSpec(memory_space=pltpu.HBM)


def of(shape, dtype):
    return jax.ShapeDtypeStruct(shape, dtype)


def kernel(body, ins, outs, shapes, limit=4, **more):
    return pl.pallas_call(
        body,
        out_shape=shapes,
        in_specs=ins,
        out_specs=outs,
        compiler_params=pltpu.CompilerParams(vmem_limit_bytes=limit * 2**20),
        **more,
    )


def on_device(gradients, master_weights, first_moment, second_moment, tensor_ids):
    me = lax.axis_index("i").astype(jnp.int32).reshape(1)
    own_f32 = pltpu.VMEM((ROWS, COLS), F32)
    chunk = pltpu.VMEM((GROUP, ROWS, COLS), BF16)

    def send(value, pairs):
        return lax.ppermute(value, "i", pairs)

    blocks = pltpu.with_memory_space_constraint(gradients.reshape(2 * CHIPS, ROWS, COLS), pltpu.HBM)
    half = pltpu.VMEM((4, GROUP, ROWS, COLS), BF16)

    def take(other):
        body = functools.partial(take_kernel, other=other)
        return kernel(
            body, [SMEM, HBM], [VMEM] * 2, [half] * 2, scratch_shapes=[pltpu.SemaphoreType.DMA((2,))]
        )(me, blocks)

    sent = take(True)
    arrived = [send(sent[k], CORE_SWAP) for k in range(2)]
    kept = take(False)
    chunks = []
    more = pltpu.VMEM((GROUP + 1, ROWS, COLS), BF16)
    for k in range(2):
        chunks += kernel(add_kernel, [VMEM] * 3, [VMEM] * 4, [more] * 4)(kept[k], arrived[k], master_weights)
    tensor, sums = kernel(
        before_kernel, [VMEM, SMEM], (VMEM, VMEM), (pltpu.VMEM((ROWS, 128), jnp.int32), pltpu.VMEM((8, 128), F32))
    )(master_weights, tensor_ids)
    wide = [send(chunks[k], shift(WIDE, offset)) for k, offset in enumerate(OFFSETS)]
    total, members = kernel(total_kernel, [VMEM] * 8, [VMEM] * 2, [chunk] * 2)(*wide, chunks[7])
    parts = exchange(total, NARROW)
    pair = send(members, shift(NARROW, (0, 1)))
    pair = kernel(join_kernel, [VMEM] * 2, VMEM, pltpu.VMEM((2, GROUP, ROWS, COLS), BF16))(members, pair)
    held = [pair] + [send(pair, shift(NARROW, (ring, 0))) for ring in RINGS[1:]]

    new_first, new_second, update, sums = kernel(
        update_kernel, [VMEM] * 6, (VMEM,) * 4, (own_f32, own_f32, own_f32, pltpu.VMEM((8, 128), F32))
    )(parts, master_weights, first_moment, second_moment, tensor, sums)

    pay = kernel(pay_kernel, [VMEM] * 2, VMEM, of((GROUP, PAY, COLS), BF16))(update, sums)
    got = exchange(pay, NARROW)
    updates = kernel(open_kernel, [VMEM], VMEM, more)(got)
    beside = send(updates, shift(WIDE, (0, 1)))
    wide = {OWN: updates, (0, 1): beside}
    for pair, value in enumerate((updates, beside)):
        for ring in RINGS[1:]:
            wide[ring, pair] = send(value, shift(WIDE, (ring, 0)))
    total = kernel(
        core_total_kernel,
        [SMEM] + [VMEM] * GROUP,
        VMEM,
        pltpu.VMEM((8, 128), F32),
        scratch_shapes=[pltpu.VMEM((GROUP, 8, 128), F32)],
    )(me, *(wide[offset] for offset in OFFSETS + (OWN,)))
    arrived = send(total, CORE_SWAP)
    trust, new_master, scaled_update = kernel(
        trust_kernel, [SMEM] + [VMEM] * 4, (VMEM,) * 3, (pltpu.VMEM((3, 8, 128), F32), own_f32, own_f32)
    )(me, total, arrived, update, master_weights)

    def params_of(offsets, values):
        body = functools.partial(params_kernel, offsets=offsets)
        shape = pltpu.VMEM((len(offsets), GROUP, ROWS, COLS), BF16)
        return kernel(body, [SMEM] + [VMEM] * (5 + len(values)), VMEM, shape)(me, trust, *values, *held)

    first, last = (OWN,) + OFFSETS[:3], OFFSETS[3:]
    params_0 = params_of(first, [wide[offset] for offset in first])
    params_1 = params_of(last, [wide[offset] for offset in last])
    other_0 = send(params_0, CORE_SWAP)
    other_1 = send(params_1, CORE_SWAP)
    every = of((2 * CHIPS, ROWS, COLS), BF16)

    def place(arrays, chunks, before=None, rows=()):
        first = before is None
        count = len(arrays) + len(rows)
        return kernel(
            functools.partial(place_kernel, arrays=len(arrays), chunks=chunks, rows=len(rows)),
            [SMEM] + [VMEM] * count + ([] if first else [HBM]),
            [HBM] * (1 + len(rows)),
            [every] + [of((ROWS, COLS), F32)] * len(rows),
            input_output_aliases={} if first else {1 + count: 0},
            scratch_shapes=[pltpu.SemaphoreType.DMA] + ([pltpu.SemaphoreType.DMA((len(rows),))] if rows else []),
        )(me, *arrays, *rows, *(() if first else (before,)))

    listed = lambda array, other, offsets: [(array, k, other, offset) for k, offset in enumerate(offsets)]
    gathered, new_first, new_second, new_master, scaled_update = place(
        [params_0, params_1],
        listed(0, False, first) + listed(1, False, last),
        rows=(new_first, new_second, new_master, scaled_update),
    )
    (gathered,) = place([other_0], listed(0, True, first), gathered)
    (gathered,) = place([other_1], listed(0, True, last), gathered)
    gathered = gathered.reshape(2 * CHIPS * ROWS, COLS)
    return (new_master, new_first, new_second, scaled_update, gathered)


def solution(mesh):
    flat = Mesh(mesh.devices.reshape(2 * CHIPS), ("i",))
    return jax.shard_map(
        on_device,
        mesh=flat,
        in_specs=(P("i", None, None), P("i", None), P("i", None), P("i", None), P("i")),
        out_specs=(P("i", None), P("i", None), P("i", None), P("i", None), P()),
        check_vma=False,
    )
```

```python
import functools

import jax
import jax.numpy as jnp
import numpy as np
from jax import lax
from jax.experimental import pallas as pl
from jax.experimental.pallas import tpu as pltpu
from jax.sharding import Mesh
from jax.sharding import PartitionSpec as P


decay_first = 0.9
decay_second = 0.999
epsilon = 1e-06
weight_decay = 0.01
step_size = 0.05


ROWS = 24
COLS = 512
CHIPS = 64
GROUP = 8
F32 = jnp.float32
BF16 = jnp.bfloat16

NUMBER = np.arange(2 * CHIPS).reshape(2, 2, 4, 4, 2)
PLACE = NUMBER.transpose(3, 2, 4, 0, 1).reshape(4, 4, 4, 2)

CORE_SWAP = [(int(a), int(b)) for pair in PLACE.reshape(CHIPS, 2) for a, b in (pair, pair[::-1])]


def grouping():
    grid = np.zeros((2, GROUP, GROUP), int)
    for core in range(2):
        for a in range(GROUP):
            for b in range(GROUP):
                x, low, z, high = (a >> 1, a & 1, b >> 1, b & 1) if core == 0 else (b >> 1, b & 1, a >> 1, a & 1)
                grid[core, a, b] = PLACE[x, 2 * high + (low ^ high), z, core]
    wide = [grid[core, :, b].tolist() for core in range(2) for b in range(GROUP)]
    narrow = [grid[core, a, :].tolist() for core in range(2) for a in range(GROUP)]
    return wide, narrow


WIDE, NARROW = grouping()


def place_of(device):
    return device >> 6, (device >> 5) & 1, (device >> 3) & 3, (device >> 1) & 3, device & 1


def group_places(device):
    z_lo, core, y, x, z_hi = place_of(device)
    p = 2 * x + ((y ^ (y >> 1)) & 1)
    q = 2 * (2 * z_hi + z_lo) + (y >> 1)
    return jnp.where(core == 0, p, q), jnp.where(core == 0, q, p)


OFFSETS = ((1, 1), (3, 1), (2, 1), (2, 0), (1, 0), (3, 0), (0, 1))
OWN = (0, 0)
HALVES = (OFFSETS[:4], OFFSETS[4:] + (OWN,))
RINGS = (0, 1, 3, 2)


def source_place(a, offset):
    ring, pair = offset
    return ((((a >> 1) + 4 - ring) & 3) << 1) + ((a & 1) ^ pair)


def target_place(a, offset):
    ring, pair = offset
    return ((((a >> 1) + ring) & 3) << 1) + ((a & 1) ^ pair)


def shift(groups, offset):
    return [(group[source_place(a, offset)], group[a]) for group in groups for a in range(GROUP)]


def owner_of(core, a, b):
    first = core == 0
    p = jnp.where(first, a, b)
    q = jnp.where(first, b, a)
    x, z = p >> 1, q >> 1
    y = 2 * (q & 1) + ((p ^ q) & 1)
    return ((z & 1) << 6) + (core << 5) + (y << 3) + (x << 1) + (z >> 1)


def exchange(value, groups):
    return lax.all_to_all(value, "i", 0, 0, axis_index_groups=groups, tiled=True)


def lane_index(rows):
    return lax.broadcasted_iota(jnp.int32, (rows, 128), 1)


def before_kernel(weights, ids, tensor, sums):
    row = lax.broadcasted_iota(jnp.int32, (ROWS, 128), 0)
    of_row = jnp.zeros((ROWS, 128), jnp.int32)
    for k in range(ROWS):
        of_row = jnp.where(row == k, ids[k], of_row)
    tensor[...] = of_row
    lane = lane_index(ROWS)
    kind = lane // 4
    w = weights[...]
    w_sq = jnp.sum(w * w, axis=1, keepdims=True)
    by_kind = jnp.where(kind == 0, w_sq, jnp.where(kind == 2, float(COLS), 0.0))
    per_tensor = jnp.sum(jnp.where(of_row == lane % 4, by_kind, 0.0), axis=0, keepdims=True)
    sums[...] = jnp.broadcast_to(per_tensor, (8, 128))


def update_kernel(parts, weights, first, second, tensor, base, new_first, new_second, update, sums):
    summed = parts[0].astype(F32)
    for k in range(1, GROUP):
        summed = summed + parts[k].astype(F32)
    m = decay_first * first[...] + (1.0 - decay_first) * summed
    v = decay_second * second[...] + (1.0 - decay_second) * summed * summed
    u = m / (jnp.sqrt(v) + epsilon) + weight_decay * weights[...]
    new_first[...] = m
    new_second[...] = v
    update[...] = u
    u_sq = jnp.sum(u * u, axis=1, keepdims=True)
    here = tensor[...] + 4 == lane_index(ROWS)
    per_tensor = jnp.sum(jnp.where(here, u_sq, 0.0), axis=0, keepdims=True)
    sums[...] = base[...] + jnp.broadcast_to(per_tensor, (8, 128))


PAY = ROWS + 8


def in_three(total):
    high = total.astype(BF16).astype(F32)
    rest = total - high
    mid = rest.astype(BF16).astype(F32)
    low = (rest - mid).astype(BF16).astype(F32)
    row = lax.broadcasted_iota(jnp.int32, (8, 128), 0)
    three = jnp.where(row == 0, high, jnp.where(row == 1, mid, jnp.where(row == 2, low, 0.0)))
    return jnp.concatenate([three, jnp.zeros((8, COLS - 128), F32)], axis=1)


def pay_kernel(update, sums, pay):
    one = jnp.concatenate([update[...], in_three(sums[0:1, :])], axis=0).astype(BF16)
    for k in range(GROUP):
        pay[k] = one


def open_kernel(got, updates):
    total = jnp.zeros((1, 128), F32)
    for k in range(GROUP):
        updates[k * ROWS : (k + 1) * ROWS] = got[k, 0:ROWS]
        three = got[k, ROWS:, 0:128].astype(F32)
        total = total + ((three[0:1] + three[1:2]) + three[2:3])
    updates[GROUP * ROWS :] = in_three(total).astype(BF16)


def trust_and_runs(total):
    update_sq = pltpu.roll(total, 124, 1)
    count = pltpu.roll(total, 120, 1)
    lane = lane_index(1)
    used = lane < 4
    trust = jnp.where(used, jnp.sqrt(total / (update_sq + count)), 0.0)
    rows = jnp.where(used, count * (1.0 / COLS), 0.0)
    start = jnp.zeros((1, 128), F32)
    for k in range(1, 4):
        start = start + jnp.where(lane >= k, pltpu.roll(rows, k, 1), 0.0)
    return trust, start, jnp.where(used, start + rows, -1.0)


def row_trust(first_row, trust, start, end):
    row = (lax.broadcasted_iota(jnp.int32, (ROWS, 128), 0) + first_row).astype(F32)
    here = jnp.logical_and(row >= start, row < end)
    return jnp.sum(jnp.where(here, trust, 0.0), axis=1, keepdims=True)


def core_total_kernel(me, *refs):
    parts, (out, totals) = refs[:GROUP], refs[GROUP:]
    place = group_places(me[0])[0]
    for part, offset in zip(parts, OFFSETS + (OWN,)):
        three = part[GROUP * ROWS :, 0:128].astype(F32)
        total = (three[0:1] + three[1:2]) + three[2:3]
        totals[source_place(place, offset)] = jnp.broadcast_to(total, (8, 128))
    total = totals[0]
    for k in range(1, GROUP):
        total = total + totals[k]
    out[...] = total


def trust_kernel(me, total, arrived, update, weights, out, new_master, scaled_update):
    three = trust_and_runs(total[0:1, :] + arrived[0:1, :])
    for k in range(3):
        out[k] = jnp.broadcast_to(three[k], (8, 128))
    scaled = row_trust(me[0] * ROWS, *three) * update[...]
    scaled_update[...] = scaled
    new_master[...] = weights[...] - step_size * scaled


def params_kernel(me, trust, *refs, offsets):
    updates, held, params = refs[: len(offsets)], refs[len(offsets) : -1], refs[-1]
    three = trust[0, 0:1, :], trust[1, 0:1, :], trust[2, 0:1, :]
    core = (me[0] >> 5) & 1
    place, place_b = group_places(me[0])
    for ring, weights in zip(RINGS, held):
        for pair in range(2):
            b = source_place(place_b, (ring, pair))
            for j, offset in enumerate(offsets):
                factor = row_trust(owner_of(core, source_place(place, offset), b) * ROWS, *three)
                member = (OFFSETS + (OWN,)).index(offset)
                block = weights[pair, member].astype(F32) - step_size * (factor * updates[j][pl.ds(pl.multiple_of(b * ROWS, 8), ROWS)].astype(F32))
                params[j, b] = block.astype(BF16)


def take_kernel(me, gradients, *refs, other):
    halves, done = refs[:2], refs[2]
    device = me[0] ^ (32 if other else 0)
    core = (device >> 5) & 1
    for k, offsets in enumerate(HALVES):
        for j, offset in enumerate(offsets):
            a = target_place(group_places(device)[0], offset)
            for b in range(GROUP):
                pltpu.make_async_copy(gradients.at[owner_of(core, a, b)], halves[k].at[j, b], done.at[k]).start()
    for k in range(2):
        pltpu.make_async_copy(halves[k], halves[k], done.at[k]).wait()


def add_kernel(kept, arrived, weights, *both):
    for j, out in enumerate(both):
        out[0:GROUP] = kept[j] + arrived[j]
        out[GROUP] = weights[...].astype(BF16)


def total_kernel(*refs):
    parts, (total, members) = refs[:-2], refs[-2:]
    for b in range(GROUP):
        summed = parts[GROUP - 1][b].astype(F32)
        for part in parts[: GROUP - 1]:
            summed = summed + part[b].astype(F32)
        total[b] = summed.astype(BF16)
    for j, part in enumerate(parts):
        members[j] = part[GROUP]


def join_kernel(*refs):
    for k, part in enumerate(refs[:-1]):
        refs[-1][k] = part[...]


def place_kernel(me, *refs, arrays, chunks, rows=0):
    blocks, whole = refs[:arrays], refs[arrays : arrays + rows]
    scratch = 1 + (rows > 0)
    outs = refs[len(refs) - scratch - 1 - rows : len(refs) - scratch]
    out, done = outs[0], refs[len(refs) - scratch]
    copies = [pltpu.make_async_copy(whole[k], outs[1 + k], refs[-1].at[k]) for k in range(rows)]
    for array, index, other, offset in chunks:
        device = me[0] ^ (32 if other else 0)
        core = (device >> 5) & 1
        a = source_place(group_places(device)[0], offset)
        part = blocks[array] if index is None else blocks[array].at[index]
        for b in range(GROUP):
            pltpu.make_async_copy(part.at[b], out.at[owner_of(core, a, b)], done).start()
    for copy in copies:
        copy.start()
    total = len(chunks) * GROUP
    pltpu.make_async_copy(out.at[pl.ds(0, total)], out.at[pl.ds(0, total)], done).wait()
    for copy in copies:
        copy.wait()


SMEM = pl.BlockSpec(memory_space=pltpu.SMEM)
VMEM = pl.BlockSpec(memory_space=pltpu.VMEM)
HBM = pl.BlockSpec(memory_space=pltpu.HBM)


def of(shape, dtype):
    return jax.ShapeDtypeStruct(shape, dtype)


def kernel(body, ins, outs, shapes, limit=4, **more):
    return pl.pallas_call(
        body,
        out_shape=shapes,
        in_specs=ins,
        out_specs=outs,
        compiler_params=pltpu.CompilerParams(vmem_limit_bytes=limit * 2**20),
        **more,
    )


def on_device(gradients, master_weights, first_moment, second_moment, tensor_ids):
    me = lax.axis_index("i").astype(jnp.int32).reshape(1)
    own_f32 = pltpu.VMEM((ROWS, COLS), F32)
    chunk = pltpu.VMEM((GROUP, ROWS, COLS), BF16)

    def send(value, pairs):
        return lax.ppermute(value, "i", pairs)

    blocks = pltpu.with_memory_space_constraint(gradients.reshape(2 * CHIPS, ROWS, COLS), pltpu.HBM)
    half = pltpu.VMEM((4, GROUP, ROWS, COLS), BF16)

    def take(other):
        body = functools.partial(take_kernel, other=other)
        return kernel(
            body, [SMEM, HBM], [VMEM] * 2, [half] * 2, scratch_shapes=[pltpu.SemaphoreType.DMA((2,))]
        )(me, blocks)

    sent = take(True)
    arrived = [send(sent[k], CORE_SWAP) for k in range(2)]
    kept = take(False)
    chunks = []
    more = pltpu.VMEM((GROUP + 1, ROWS, COLS), BF16)
    for k in range(2):
        chunks += kernel(add_kernel, [VMEM] * 3, [VMEM] * 4, [more] * 4)(kept[k], arrived[k], master_weights)
    tensor, sums = kernel(
        before_kernel, [VMEM, SMEM], (VMEM, VMEM), (pltpu.VMEM((ROWS, 128), jnp.int32), pltpu.VMEM((8, 128), F32))
    )(master_weights, tensor_ids)
    wide = [send(chunks[k], shift(WIDE, offset)) for k, offset in enumerate(OFFSETS)]
    total, members = kernel(total_kernel, [VMEM] * 8, [VMEM] * 2, [chunk] * 2)(*wide, chunks[7])
    parts = exchange(total, NARROW)
    pair = send(members, shift(NARROW, (0, 1)))
    pair = kernel(join_kernel, [VMEM] * 2, VMEM, pltpu.VMEM((2, GROUP, ROWS, COLS), BF16))(members, pair)
    held = [pair] + [send(pair, shift(NARROW, (ring, 0))) for ring in RINGS[1:]]

    new_first, new_second, update, sums = kernel(
        update_kernel, [VMEM] * 6, (VMEM,) * 4, (own_f32, own_f32, own_f32, pltpu.VMEM((8, 128), F32))
    )(parts, master_weights, first_moment, second_moment, tensor, sums)

    pay = kernel(pay_kernel, [VMEM] * 2, VMEM, of((GROUP, PAY, COLS), BF16))(update, sums)
    got = exchange(pay, NARROW)
    updates = kernel(open_kernel, [VMEM], VMEM, pltpu.VMEM((GROUP * ROWS + 8, COLS), BF16))(got)
    beside = send(updates, shift(WIDE, (0, 1)))
    wide = {OWN: updates, (0, 1): beside}
    for pair, value in enumerate((updates, beside)):
        for ring in RINGS[1:]:
            wide[ring, pair] = send(value, shift(WIDE, (ring, 0)))
    total = kernel(
        core_total_kernel,
        [SMEM] + [VMEM] * GROUP,
        VMEM,
        pltpu.VMEM((8, 128), F32),
        scratch_shapes=[pltpu.VMEM((GROUP, 8, 128), F32)],
    )(me, *(wide[offset] for offset in OFFSETS + (OWN,)))
    arrived = send(total, CORE_SWAP)
    trust, new_master, scaled_update = kernel(
        trust_kernel, [SMEM] + [VMEM] * 4, (VMEM,) * 3, (pltpu.VMEM((3, 8, 128), F32), own_f32, own_f32)
    )(me, total, arrived, update, master_weights)

    def params_of(offsets, values):
        body = functools.partial(params_kernel, offsets=offsets)
        shape = pltpu.VMEM((len(offsets), GROUP, ROWS, COLS), BF16)
        return kernel(body, [SMEM] + [VMEM] * (5 + len(values)), VMEM, shape)(me, trust, *values, *held)

    first, last = (OWN,) + OFFSETS[:3], OFFSETS[3:]
    params_0 = params_of(first, [wide[offset] for offset in first])
    params_1 = params_of(last, [wide[offset] for offset in last])
    other_0 = send(params_0, CORE_SWAP)
    other_1 = send(params_1, CORE_SWAP)
    every = of((2 * CHIPS, ROWS, COLS), BF16)

    def place(arrays, chunks, before=None, rows=()):
        first = before is None
        count = len(arrays) + len(rows)
        return kernel(
            functools.partial(place_kernel, arrays=len(arrays), chunks=chunks, rows=len(rows)),
            [SMEM] + [VMEM] * count + ([] if first else [HBM]),
            [HBM] * (1 + len(rows)),
            [every] + [of((ROWS, COLS), F32)] * len(rows),
            input_output_aliases={} if first else {1 + count: 0},
            scratch_shapes=[pltpu.SemaphoreType.DMA] + ([pltpu.SemaphoreType.DMA((len(rows),))] if rows else []),
        )(me, *arrays, *rows, *(() if first else (before,)))

    listed = lambda array, other, offsets: [(array, k, other, offset) for k, offset in enumerate(offsets)]
    gathered, new_first, new_second, new_master, scaled_update = place(
        [params_0, params_1],
        listed(0, False, first) + listed(1, False, last),
        rows=(new_first, new_second, new_master, scaled_update),
    )
    (gathered,) = place([other_0], listed(0, True, first), gathered)
    (gathered,) = place([other_1], listed(0, True, last), gathered)
    gathered = gathered.reshape(2 * CHIPS * ROWS, COLS)
    return (new_master, new_first, new_second, scaled_update, gathered)


def solution(mesh):
    flat = Mesh(mesh.devices.reshape(2 * CHIPS), ("i",))
    return jax.shard_map(
        on_device,
        mesh=flat,
        in_specs=(P("i", None, None), P("i", None), P("i", None), P("i", None), P("i")),
        out_specs=(P("i", None), P("i", None), P("i", None), P("i", None), P()),
        check_vma=False,
    )
```

```python
import functools

import jax
import jax.numpy as jnp
import numpy as np
from jax import lax
from jax.experimental import pallas as pl
from jax.experimental.pallas import tpu as pltpu
from jax.sharding import Mesh
from jax.sharding import PartitionSpec as P


decay_first = 0.9
decay_second = 0.999
epsilon = 1e-06
weight_decay = 0.01
step_size = 0.05


ROWS = 24
COLS = 512
CHIPS = 64
GROUP = 8
F32 = jnp.float32
BF16 = jnp.bfloat16

NUMBER = np.arange(2 * CHIPS).reshape(2, 2, 4, 4, 2)
PLACE = NUMBER.transpose(3, 2, 4, 0, 1).reshape(4, 4, 4, 2)

CORE_SWAP = [(int(a), int(b)) for pair in PLACE.reshape(CHIPS, 2) for a, b in (pair, pair[::-1])]


def grouping():
    grid = np.zeros((2, GROUP, GROUP), int)
    for core in range(2):
        for a in range(GROUP):
            for b in range(GROUP):
                x, low, z, high = (a >> 1, a & 1, b >> 1, b & 1) if core == 0 else (b >> 1, b & 1, a >> 1, a & 1)
                grid[core, a, b] = PLACE[x, 2 * high + (low ^ high), z, core]
    wide = [grid[core, :, b].tolist() for core in range(2) for b in range(GROUP)]
    narrow = [grid[core, a, :].tolist() for core in range(2) for a in range(GROUP)]
    return wide, narrow


WIDE, NARROW = grouping()


def place_of(device):
    return device >> 6, (device >> 5) & 1, (device >> 3) & 3, (device >> 1) & 3, device & 1


def group_places(device):
    z_lo, core, y, x, z_hi = place_of(device)
    p = 2 * x + ((y ^ (y >> 1)) & 1)
    q = 2 * (2 * z_hi + z_lo) + (y >> 1)
    return jnp.where(core == 0, p, q), jnp.where(core == 0, q, p)


OFFSETS = ((1, 1), (3, 1), (2, 0), (2, 1), (0, 1), (1, 0), (3, 0))
OWN = (0, 0)
HALVES = (OFFSETS[:3], OFFSETS[3:] + (OWN,))
RINGS = (0, 1, 3, 2)


def source_place(a, offset):
    ring, pair = offset
    return ((((a >> 1) + 4 - ring) & 3) << 1) + ((a & 1) ^ pair)


def target_place(a, offset):
    ring, pair = offset
    return ((((a >> 1) + ring) & 3) << 1) + ((a & 1) ^ pair)


def shift(groups, offset):
    return [(group[source_place(a, offset)], group[a]) for group in groups for a in range(GROUP)]


def owner_of(core, a, b):
    first = core == 0
    p = jnp.where(first, a, b)
    q = jnp.where(first, b, a)
    x, z = p >> 1, q >> 1
    y = 2 * (q & 1) + ((p ^ q) & 1)
    return ((z & 1) << 6) + (core << 5) + (y << 3) + (x << 1) + (z >> 1)


def exchange(value, groups):
    return lax.all_to_all(value, "i", 0, 0, axis_index_groups=groups, tiled=True)


def lane_index(rows):
    return lax.broadcasted_iota(jnp.int32, (rows, 128), 1)


def before_kernel(weights, ids, tensor, sums):
    row = lax.broadcasted_iota(jnp.int32, (ROWS, 128), 0)
    of_row = jnp.zeros((ROWS, 128), jnp.int32)
    for k in range(ROWS):
        of_row = jnp.where(row == k, ids[k], of_row)
    tensor[...] = of_row
    lane = lane_index(ROWS)
    kind = lane // 4
    w = weights[...]
    w_sq = jnp.sum(w * w, axis=1, keepdims=True)
    by_kind = jnp.where(kind == 0, w_sq, jnp.where(kind == 2, float(COLS), 0.0))
    per_tensor = jnp.sum(jnp.where(of_row == lane % 4, by_kind, 0.0), axis=0, keepdims=True)
    sums[...] = jnp.broadcast_to(per_tensor, (8, 128))


def update_kernel(parts, weights, first, second, tensor, base, new_first, new_second, update, sums):
    summed = parts[0].astype(F32)
    for k in range(1, GROUP):
        summed = summed + parts[k].astype(F32)
    m = decay_first * first[...] + (1.0 - decay_first) * summed
    v = decay_second * second[...] + (1.0 - decay_second) * summed * summed
    u = m / (jnp.sqrt(v) + epsilon) + weight_decay * weights[...]
    new_first[...] = m
    new_second[...] = v
    update[...] = u
    u_sq = jnp.sum(u * u, axis=1, keepdims=True)
    here = tensor[...] + 4 == lane_index(ROWS)
    per_tensor = jnp.sum(jnp.where(here, u_sq, 0.0), axis=0, keepdims=True)
    sums[...] = base[...] + jnp.broadcast_to(per_tensor, (8, 128))


PAY = ROWS + 8


def in_three(total):
    high = total.astype(BF16).astype(F32)
    rest = total - high
    mid = rest.astype(BF16).astype(F32)
    low = (rest - mid).astype(BF16).astype(F32)
    row = lax.broadcasted_iota(jnp.int32, (8, 128), 0)
    three = jnp.where(row == 0, high, jnp.where(row == 1, mid, jnp.where(row == 2, low, 0.0)))
    return jnp.concatenate([three, jnp.zeros((8, COLS - 128), F32)], axis=1)


def pay_kernel(update, sums, pay):
    one = jnp.concatenate([update[...], in_three(sums[0:1, :])], axis=0).astype(BF16)
    for k in range(GROUP):
        pay[k] = one


def open_kernel(got, updates):
    total = jnp.zeros((1, 128), F32)
    for k in range(GROUP):
        updates[k * ROWS : (k + 1) * ROWS] = got[k, 0:ROWS]
        three = got[k, ROWS:, 0:128].astype(F32)
        total = total + ((three[0:1] + three[1:2]) + three[2:3])
    updates[GROUP * ROWS :] = in_three(total).astype(BF16)


def trust_and_runs(total):
    update_sq = pltpu.roll(total, 124, 1)
    count = pltpu.roll(total, 120, 1)
    lane = lane_index(1)
    used = lane < 4
    trust = jnp.where(used, jnp.sqrt(total / (update_sq + count)), 0.0)
    rows = jnp.where(used, count * (1.0 / COLS), 0.0)
    start = jnp.zeros((1, 128), F32)
    for k in range(1, 4):
        start = start + jnp.where(lane >= k, pltpu.roll(rows, k, 1), 0.0)
    return trust, start, jnp.where(used, start + rows, -1.0)


def row_trust(first_row, trust, start, end):
    row = (lax.broadcasted_iota(jnp.int32, (ROWS, 128), 0) + first_row).astype(F32)
    here = jnp.logical_and(row >= start, row < end)
    return jnp.sum(jnp.where(here, trust, 0.0), axis=1, keepdims=True)


def core_total_kernel(me, *refs):
    parts, (out, totals) = refs[:GROUP], refs[GROUP:]
    place = group_places(me[0])[0]
    for part, offset in zip(parts, OFFSETS + (OWN,)):
        three = part[GROUP * ROWS :, 0:128].astype(F32)
        total = (three[0:1] + three[1:2]) + three[2:3]
        totals[source_place(place, offset)] = jnp.broadcast_to(total, (8, 128))
    total = totals[0]
    for k in range(1, GROUP):
        total = total + totals[k]
    out[...] = total


def trust_kernel(me, total, arrived, update, weights, out, new_master, scaled_update):
    three = trust_and_runs(total[0:1, :] + arrived[0:1, :])
    for k in range(3):
        out[k] = jnp.broadcast_to(three[k], (8, 128))
    scaled = row_trust(me[0] * ROWS, *three) * update[...]
    scaled_update[...] = scaled
    new_master[...] = weights[...] - step_size * scaled


def params_kernel(me, trust, *refs, offsets):
    updates, held, params = refs[: len(offsets)], refs[len(offsets) : -1], refs[-1]
    three = trust[0, 0:1, :], trust[1, 0:1, :], trust[2, 0:1, :]
    core = (me[0] >> 5) & 1
    place, place_b = group_places(me[0])
    for ring, weights in zip(RINGS, held):
        for pair in range(2):
            b = source_place(place_b, (ring, pair))
            for j, offset in enumerate(offsets):
                factor = row_trust(owner_of(core, source_place(place, offset), b) * ROWS, *three)
                member = (OFFSETS + (OWN,)).index(offset)
                block = weights[pair, member].astype(F32) - step_size * (factor * updates[j][pl.ds(pl.multiple_of(b * ROWS, 8), ROWS)].astype(F32))
                params[j, b] = block.astype(BF16)


def take_kernel(me, gradients, *refs, other):
    halves, done = refs[:2], refs[2]
    device = me[0] ^ (32 if other else 0)
    core = (device >> 5) & 1
    for k, offsets in enumerate(HALVES):
        for j, offset in enumerate(offsets):
            a = target_place(group_places(device)[0], offset)
            for b in range(GROUP):
                pltpu.make_async_copy(gradients.at[owner_of(core, a, b)], halves[k].at[j, b], done.at[k]).start()
    for k in range(2):
        pltpu.make_async_copy(halves[k], halves[k], done.at[k]).wait()


def add_kernel(kept, arrived, weights, *both):
    for j, out in enumerate(both):
        out[0:GROUP] = kept[j] + arrived[j]
        out[GROUP] = weights[...].astype(BF16)


def total_kernel(*refs):
    parts, (total, members) = refs[:-2], refs[-2:]
    for b in range(GROUP):
        summed = parts[GROUP - 1][b].astype(F32)
        for part in parts[: GROUP - 1]:
            summed = summed + part[b].astype(F32)
        total[b] = summed.astype(BF16)
    for j, part in enumerate(parts):
        members[j] = part[GROUP]


def join_kernel(*refs):
    for k, part in enumerate(refs[:-1]):
        refs[-1][k] = part[...]


def place_kernel(me, *refs, arrays, chunks, rows=0):
    blocks, whole = refs[:arrays], refs[arrays : arrays + rows]
    scratch = 1 + (rows > 0)
    outs = refs[len(refs) - scratch - 1 - rows : len(refs) - scratch]
    out, done = outs[0], refs[len(refs) - scratch]
    copies = [pltpu.make_async_copy(whole[k], outs[1 + k], refs[-1].at[k]) for k in range(rows)]
    for array, index, other, offset in chunks:
        device = me[0] ^ (32 if other else 0)
        core = (device >> 5) & 1
        a = source_place(group_places(device)[0], offset)
        part = blocks[array] if index is None else blocks[array].at[index]
        for b in range(GROUP):
            pltpu.make_async_copy(part.at[b], out.at[owner_of(core, a, b)], done).start()
    for copy in copies:
        copy.start()
    total = len(chunks) * GROUP
    pltpu.make_async_copy(out.at[pl.ds(0, total)], out.at[pl.ds(0, total)], done).wait()
    for copy in copies:
        copy.wait()


SMEM = pl.BlockSpec(memory_space=pltpu.SMEM)
VMEM = pl.BlockSpec(memory_space=pltpu.VMEM)
HBM = pl.BlockSpec(memory_space=pltpu.HBM)


def of(shape, dtype):
    return jax.ShapeDtypeStruct(shape, dtype)


def kernel(body, ins, outs, shapes, limit=4, **more):
    return pl.pallas_call(
        body,
        out_shape=shapes,
        in_specs=ins,
        out_specs=outs,
        compiler_params=pltpu.CompilerParams(vmem_limit_bytes=limit * 2**20),
        **more,
    )


def on_device(gradients, master_weights, first_moment, second_moment, tensor_ids):
    me = lax.axis_index("i").astype(jnp.int32).reshape(1)
    own_f32 = pltpu.VMEM((ROWS, COLS), F32)
    chunk = pltpu.VMEM((GROUP, ROWS, COLS), BF16)

    def send(value, pairs):
        return lax.ppermute(value, "i", pairs)

    blocks = pltpu.with_memory_space_constraint(gradients.reshape(2 * CHIPS, ROWS, COLS), pltpu.HBM)
    half = [pltpu.VMEM((len(offsets), GROUP, ROWS, COLS), BF16) for offsets in HALVES]

    def take(other):
        body = functools.partial(take_kernel, other=other)
        return kernel(body, [SMEM, HBM], [VMEM] * 2, half, scratch_shapes=[pltpu.SemaphoreType.DMA((2,))])(me, blocks)

    sent = take(True)
    arrived = [send(sent[k], CORE_SWAP) for k in range(2)]
    kept = take(False)
    chunks = []
    more = pltpu.VMEM((GROUP + 1, ROWS, COLS), BF16)
    for k in range(2):
        chunks += kernel(add_kernel, [VMEM] * 3, [VMEM] * len(HALVES[k]), [more] * len(HALVES[k]))(
            kept[k], arrived[k], master_weights
        )
    tensor, sums = kernel(
        before_kernel, [VMEM, SMEM], (VMEM, VMEM), (pltpu.VMEM((ROWS, 128), jnp.int32), pltpu.VMEM((8, 128), F32))
    )(master_weights, tensor_ids)
    wide = [send(chunks[k], shift(WIDE, offset)) for k, offset in enumerate(OFFSETS)]
    total, members = kernel(total_kernel, [VMEM] * 8, [VMEM] * 2, [chunk] * 2)(*wide, chunks[7])
    parts = exchange(total, NARROW)
    pair = send(members, shift(NARROW, (0, 1)))
    pair = kernel(join_kernel, [VMEM] * 2, VMEM, pltpu.VMEM((2, GROUP, ROWS, COLS), BF16))(members, pair)
    held = [pair] + [send(pair, shift(NARROW, (ring, 0))) for ring in RINGS[1:]]

    new_first, new_second, update, sums = kernel(
        update_kernel, [VMEM] * 6, (VMEM,) * 4, (own_f32, own_f32, own_f32, pltpu.VMEM((8, 128), F32))
    )(parts, master_weights, first_moment, second_moment, tensor, sums)

    pay = kernel(pay_kernel, [VMEM] * 2, VMEM, of((GROUP, PAY, COLS), BF16))(update, sums)
    got = exchange(pay, NARROW)
    updates = kernel(open_kernel, [VMEM], VMEM, pltpu.VMEM((GROUP * ROWS + 8, COLS), BF16))(got)
    beside = send(updates, shift(WIDE, (0, 1)))
    wide = {OWN: updates, (0, 1): beside}
    for pair, value in enumerate((updates, beside)):
        for ring in RINGS[1:]:
            wide[ring, pair] = send(value, shift(WIDE, (ring, 0)))
    total = kernel(
        core_total_kernel,
        [SMEM] + [VMEM] * GROUP,
        VMEM,
        pltpu.VMEM((8, 128), F32),
        scratch_shapes=[pltpu.VMEM((GROUP, 8, 128), F32)],
    )(me, *(wide[offset] for offset in OFFSETS + (OWN,)))
    arrived = send(total, CORE_SWAP)
    trust, new_master, scaled_update = kernel(
        trust_kernel, [SMEM] + [VMEM] * 4, (VMEM,) * 3, (pltpu.VMEM((3, 8, 128), F32), own_f32, own_f32)
    )(me, total, arrived, update, master_weights)

    def params_of(offsets, values):
        body = functools.partial(params_kernel, offsets=offsets)
        shape = pltpu.VMEM((len(offsets), GROUP, ROWS, COLS), BF16)
        return kernel(body, [SMEM] + [VMEM] * (5 + len(values)), VMEM, shape)(me, trust, *values, *held)

    first, last = (OWN,) + OFFSETS[:3], OFFSETS[3:]
    params_0 = params_of(first, [wide[offset] for offset in first])
    params_1 = params_of(last, [wide[offset] for offset in last])
    other_0 = send(params_0, CORE_SWAP)
    other_1 = send(params_1, CORE_SWAP)
    every = of((2 * CHIPS, ROWS, COLS), BF16)

    def place(arrays, chunks, before=None, rows=()):
        first = before is None
        count = len(arrays) + len(rows)
        return kernel(
            functools.partial(place_kernel, arrays=len(arrays), chunks=chunks, rows=len(rows)),
            [SMEM] + [VMEM] * count + ([] if first else [HBM]),
            [HBM] * (1 + len(rows)),
            [every] + [of((ROWS, COLS), F32)] * len(rows),
            input_output_aliases={} if first else {1 + count: 0},
            scratch_shapes=[pltpu.SemaphoreType.DMA] + ([pltpu.SemaphoreType.DMA((len(rows),))] if rows else []),
        )(me, *arrays, *rows, *(() if first else (before,)))

    listed = lambda array, other, offsets: [(array, k, other, offset) for k, offset in enumerate(offsets)]
    gathered, new_first, new_second, new_master, scaled_update = place(
        [params_0, params_1],
        listed(0, False, first) + listed(1, False, last),
        rows=(new_first, new_second, new_master, scaled_update),
    )
    (gathered,) = place([other_0], listed(0, True, first), gathered)
    (gathered,) = place([other_1], listed(0, True, last), gathered)
    gathered = gathered.reshape(2 * CHIPS * ROWS, COLS)
    return (new_master, new_first, new_second, scaled_update, gathered)


def solution(mesh):
    flat = Mesh(mesh.devices.reshape(2 * CHIPS), ("i",))
    return jax.shard_map(
        on_device,
        mesh=flat,
        in_specs=(P("i", None, None), P("i", None), P("i", None), P("i", None), P("i")),
        out_specs=(P("i", None), P("i", None), P("i", None), P("i", None), P()),
        check_vma=False,
    )
```
